32 devices in a mesh: groups: 2 (over y), section: 4 (over z), seq: 4 (over x, core).
Axes of the slice: x: 2, y: 2, z: 4, core: 2. Of those that a mesh axis runs over, the one named last changes fastest.
Arguments:
- tokens: bfloat16 [8, 256, 1440], P('groups', 'seq'), parts along dimension 0, may hold values from -6 to 6
- block_order: int32 [8], P('groups'), parts along dimension 0, may hold values from 0 to 3, each once
- prompt_lengths: int32 [8], P('groups'), parts along dimension 0, may hold values from 1 to 256, 576 in all
- norm_gain: float32 [4, 1440], P('section'), may hold values from 0.1 to 1.9
- w_query: bfloat16 [4, 1440, 2048], P('section', None, 'seq'), may hold values from -4 to 4
- w_key_value: bfloat16 [4, 1440, 512], P('section'), may hold values from -4 to 4
- w_out: bfloat16 [4, 2048, 1440], P('section', 'seq'), may hold values from -0.125 to 0.125
- sink_logits: float32 [4, 32], P('section'), may hold values from 0 to 4
Outputs:
- hidden_states: bfloat16 [4, 8, 256, 1440], P('section', 'groups', 'seq'), parts along dimension 1
- layer_cache: bfloat16 [4, 8, 256, 512], P('section', 'groups', 'seq'), parts along dimension 1
The draws below stay inside these ranges and needn't reach their ends.
There are 2 independent parts, one for each index of `groups`. The reference program is written for one: setup_inputs(seed, part) draws one part's arguments, and reference() takes and returns one part's arrays. A program takes and returns all parts, laid end to end along the dimension named above; an argument that names none is the same for every part. Nothing has to cross between parts.
Inputs may be any that keep to these rules, and one draw needn't show every extreme that they name: `block_order`: each of 0 to 3 exactly once. `prompt_lengths`: the longest prompt is full.
All inputs are finite; a program needn't handle non-finite values.
Results may differ from the reference program's by a relative error of at most 0.024.
Values may be sent and summed in bfloat16 or wider, within the bound.
A program may use at most 128 MiB of HBM per device.

```python
import math
import jax
import jax.numpy as jnp
import numpy as np
from jax import lax

D = 1440
HEADS = 32
KV_HEADS = 4
HEAD_DIM = 64
WIN = 128
MICRO = 4
BLOCK = 256
LAYERS = 4


def base_keys(key):
    drawn = jax.random.normal(jax.random.fold_in(key, 7), (LAYERS, D, 2 * KV_HEADS * HEAD_DIM), jnp.float32)
    return drawn * D ** (-0.5)


def draw_w_key_value(key, part):
    return jnp.clip(base_keys(key), -4.0, 4.0).astype(jnp.bfloat16)


def draw_w_query(key, part):
    drawn = jax.random.normal(jax.random.fold_in(key, 1), (LAYERS, D, HEADS * HEAD_DIM), jnp.float32) * D ** (-0.5)
    return jnp.clip(drawn, -4.0, 4.0).astype(jnp.bfloat16)


def steps_of(own_key, extent, cuts, least, top_value):
    def one(position, blocks):
        heights = jax.random.uniform(jax.random.fold_in(jax.random.fold_in(own_key, 6), position), (blocks,), jnp.float32, least / len(cuts), top_value / len(cuts))
        return jnp.repeat(jnp.exp(heights), extent[position] // blocks).reshape((-1,) + (1,) * (len(extent) - position - 1))

    loudness = one(*cuts[0])
    for cut in cuts[1:]:
        loudness = loudness * one(*cut)
    return loudness


def length_profile(count, total, limit, lean):
    loads = [(1 << 20) // math.isqrt(rank ** lean) + 1 for rank in range(2, count + 1)]
    surplus, holding = total - limit - (count - 1), [1] * (count - 1)
    while surplus > 0:
        free = [i for i in range(count - 1) if holding[i] < limit]
        whole, left = sum([loads[i] for i in free]), surplus
        for i in free:
            addition = min(limit - holding[i], max(1, left * loads[i] // whole), surplus)
            holding[i] = holding[i] + addition
            surplus = surplus - addition
    return np.array([limit] + holding)


def uneven_parts(key, amount, total, most, lean):
    if amount == 2:
        one = jax.random.randint(key, (), max(1, total - most), min(most, total - 1) + 1)
        return jnp.stack([one, total - one])
    tallies = jnp.asarray(length_profile(amount, total, most, lean), jnp.int32)
    couples = (amount - 1) // 2
    giver, receiver = tallies[1:1 + 2 * couples:2], tallies[2:2 + 2 * couples:2]
    margin = jnp.minimum(giver - 1, most - receiver)
    shifted = jax.random.randint(jax.random.fold_in(key, 1), (couples,), 0, 1 << 20) % (margin + 1)
    tallies = tallies.at[1:1 + 2 * couples:2].set(giver - shifted).at[2:2 + 2 * couples:2].set(receiver + shifted)
    return tallies[jax.random.permutation(jax.random.fold_in(key, 2), amount)]


def noise(rng, shape, spread, reach, pieces=(), kind=jnp.bfloat16):
    level = steps_of(rng, shape, pieces, -0.22, 0.18) if pieces else 1.0
    entries = jax.random.normal(rng, shape, jnp.float32) * spread * level
    return jnp.minimum(jnp.maximum(entries, -reach), reach).astype(kind)


def setup_inputs(seed: int = 0, part: int = 0) -> dict:
    arg_keys = jax.random.split(jax.random.key(seed), 9)
    part_keys = jax.random.split(jax.random.fold_in(arg_keys[8], part), 9)
    tokens = noise(part_keys[0], (MICRO, BLOCK, D), 1.0, 6.0, ((1, 4),))
    block_order = jax.random.permutation(part_keys[1], MICRO).astype(jnp.int32)
    prompt_lengths = uneven_parts(part_keys[2], MICRO, 9 * MICRO * BLOCK // 16, BLOCK, 2).astype(jnp.int32)
    norm_gain = jnp.clip(1.0 + 0.18 * jax.random.normal(arg_keys[3], (LAYERS, D), jnp.float32), 0.1, 1.9)
    w_query = draw_w_query(jax.random.fold_in(arg_keys[8], 71), part)
    w_key_value = draw_w_key_value(jax.random.fold_in(arg_keys[8], 71), part)
    w_out = noise(arg_keys[6], (LAYERS, HEADS * HEAD_DIM, D), (HEADS * HEAD_DIM) ** -0.5, 0.125, ((0, 4), (1, 4)))
    sink_logits = jnp.clip(4.0 * jax.random.uniform(arg_keys[7], (LAYERS, HEADS), jnp.float32) ** steps_of(arg_keys[7], (LAYERS, HEADS), ((0, 4),), -0.2, 0.2), 0.0, 4.0)
    return dict(tokens=tokens, block_order=block_order, prompt_lengths=prompt_lengths, norm_gain=norm_gain, w_query=w_query, w_key_value=w_key_value, w_out=w_out, sink_logits=sink_logits)


THETA = 150000.0
EPSILON = 1e-05

def rotary(positions, head_size):
    half = head_size // 2
    freq = jnp.exp(jnp.arange(half, dtype=jnp.float32) * (-2.0 * math.log(THETA) / head_size))
    angles = positions.astype(jnp.float32)[:, None] * freq[None, :]
    return (jnp.cos(angles)[:, None, :], jnp.sin(angles)[:, None, :])

def rotate(values, cosine, sine):
    half = values.shape[-1] // 2
    first = values[..., :half]
    second = values[..., half:]
    return jnp.concatenate([first * cosine - second * sine, second * cosine + first * sine], -1)

def layer_step(hidden, gain, w_query, w_key_value, w_out, sinks, cosine, sine, allowed):
    group = HEADS // KV_HEADS
    kv_width = KV_HEADS * HEAD_DIM
    count = hidden.shape[0]
    widened = hidden.astype(jnp.float32)
    scale = lax.rsqrt(lax.optimization_barrier(jnp.mean(widened * widened, -1, keepdims=True)) + EPSILON)
    normed = (widened * scale * gain).astype(jnp.bfloat16)
    queries = jnp.dot(normed, w_query, preferred_element_type=jnp.float32).reshape(count, HEADS, HEAD_DIM)
    queries = rotate(queries, cosine, sine).astype(jnp.bfloat16)
    projected = jnp.dot(normed, w_key_value, preferred_element_type=jnp.float32)
    keys = rotate(projected[:, :kv_width].reshape(count, KV_HEADS, HEAD_DIM), cosine, sine).reshape(count, kv_width)
    cache = jnp.concatenate([keys, projected[:, kv_width:]], 1).astype(jnp.bfloat16)
    key_heads = cache[:, :kv_width].reshape(count, KV_HEADS, HEAD_DIM).astype(jnp.float32)
    value_heads = cache[:, kv_width:].reshape(count, KV_HEADS, HEAD_DIM).astype(jnp.float32)
    grouped = queries.reshape(count, KV_HEADS, group, HEAD_DIM).astype(jnp.float32)
    scores = jnp.einsum('qkgd,skd->kgqs', grouped, key_heads) * 0.125
    sink = sinks.reshape(KV_HEADS, group)[:, :, None]
    masked = jnp.where(allowed, scores, jnp.float32(-1e+30))
    top = jnp.maximum(lax.optimization_barrier(jnp.max(masked, -1)), sink)
    expo = jnp.where(allowed, jnp.exp(scores - top[..., None]), jnp.float32(0.0))
    total = lax.optimization_barrier(jnp.sum(expo, -1)) + jnp.exp(sink - top)
    weights = (expo / total[..., None]).astype(jnp.bfloat16)
    context = jnp.einsum('kgqs,skd->qkgd', weights.astype(jnp.float32), value_heads)
    context = context.reshape(count, HEADS * HEAD_DIM).astype(jnp.bfloat16)
    output = jnp.dot(context, w_out, preferred_element_type=jnp.float32)
    return ((widened + output).astype(jnp.bfloat16), cache)

def reference(tokens, block_order, prompt_lengths, norm_gain, w_query, w_key_value, w_out, sink_logits):
    positions = jnp.arange(BLOCK, dtype=jnp.int32)
    cosine, sine = rotary(positions, HEAD_DIM)
    within = (positions[None, :] <= positions[:, None]) & (positions[:, None] - positions[None, :] < WIN)
    hidden_rows = [[] for layer in range(LAYERS)]
    cache_rows = [[] for layer in range(LAYERS)]
    for slot in range(MICRO):
        block = block_order[slot]
        hidden = lax.dynamic_index_in_dim(tokens, block, 0, keepdims=False)
        length = lax.dynamic_index_in_dim(prompt_lengths, block, 0, keepdims=False)
        allowed = within & ((positions[None, :] < length) | (positions[None, :] == positions[:, None]))
        for layer in range(LAYERS):
            hidden, cache = layer_step(hidden, norm_gain[layer], w_query[layer], w_key_value[layer], w_out[layer], sink_logits[layer], cosine, sine, allowed)
            hidden_rows[layer].append(hidden)
            cache_rows[layer].append(cache)
    hidden_states = jnp.stack([jnp.stack(row) for row in hidden_rows])
    layer_cache = jnp.stack([jnp.stack(row) for row in cache_rows])
    return (hidden_states, layer_cache)
```

```python
import functools
import math

import jax
import jax.numpy as jnp
from jax import lax
from jax.experimental import pallas as pl
from jax.experimental.pallas import tpu as pltpu
from jax.sharding import PartitionSpec as P

HEAD_DIM = 64
WIN = 128
LANES = 128
THETA = 150000.0
EPSILON = 1e-05
MESH = pl.DeviceIdType.MESH
F32 = jnp.float32
BF16 = jnp.bfloat16
QUERY_CUTS = 5
OUT_STEP = 256
HOP_CUTS = 3


def kernel(
    shape,
    order_ref, length_ref, sink_ref,
    tokens_hbm, gain_hbm, pair_hbm, query_hbm, out_hbm,
    hidden_ref, cache_ref,
    tokens_ref, gain_ref, pair_ref, out_t, cos_tab, sin_tab,
    query_w, out_w, arrive, window, hbuf, normed_ref, qbuf, cbuf, sink_rows,
    gathered, tq, kd_buf, vd_buf, ctx, outgoing, incoming, final, acc,
    local_sem, x_send, x_recv, y_send, y_recv, d_send, d_recv, own_send, own_recv,
    w_send, w_recv, z_send, z_recv,
    ax_send, ax_recv, ad_send, ad_recv, rd_send, rd_recv, rx_send, rx_recv,
):
    groups, sections, seq = shape
    chips = seq // 2
    g = lax.axis_index("groups")
    sec = lax.axis_index("section")
    q = lax.axis_index("seq")
    chip, core = q // 2, q % 2
    partner = chip * 2 + (1 - core)
    micro, rows, width = hidden_ref.shape
    shard = query_w.shape[2]
    heads_width = seq * shard
    kv_width = pair_ref.shape[1] // 2
    kv_heads = kv_width // HEAD_DIM
    group = heads_width // kv_width
    keep = min(WIN, rows)
    depth = WIN // keep
    span = WIN + rows
    total = seq * rows
    half = HEAD_DIM // 2
    own_heads = shard // HEAD_DIM

    query_size = width // groups // QUERY_CUTS
    out_rows = shard // groups
    out_edges = [(c, min(OUT_STEP, width - c)) for c in range(0, width, OUT_STEP)]
    cuts = (QUERY_CUTS, len(out_edges))

    def query_load(j, k):
        first = pl.multiple_of((((g + j) % groups) * QUERY_CUTS + k) * query_size, 16)
        return pltpu.make_async_copy(
            query_hbm.at[pl.ds(first, query_size)], query_w.at[q, pl.ds(first, query_size)],
            local_sem.at[j * QUERY_CUTS + k],
        )

    base = groups * QUERY_CUTS
    out_load = pltpu.make_async_copy(out_hbm, out_t, local_sem.at[base])
    pair_load = pltpu.make_async_copy(pair_hbm, pair_ref, local_sem.at[base + 1])
    gain_load = pltpu.make_async_copy(gain_hbm, gain_ref, local_sem.at[base + 2])
    tokens_load = pltpu.make_async_copy(tokens_hbm, tokens_ref, local_sem.at[base + 3])

    @pl.when(sec == 0)
    def _():
        gain_load.start()
        tokens_load.start()

    for j in range(groups):
        for k in range(QUERY_CUTS):
            query_load(j, k).start()
    out_load.start()
    pair_load.start()

    @pl.when(sec > 0)
    def _():
        gain_load.start()

    barrier = pltpu.get_barrier_semaphore()
    greeted = 0
    for d in range(1, seq):
        pl.semaphore_signal(barrier, 1, device_id={"seq": (q + d) % seq}, device_id_type=MESH)
        greeted += 1
    for e in range(1, groups):
        pl.semaphore_signal(barrier, 1, device_id={"groups": (g + e) % groups}, device_id_type=MESH)
        greeted += 1
    for s in sorted({1 % sections, (sections - 1) % sections} - {0}):
        pl.semaphore_signal(barrier, 1, device_id={"section": (sec + s) % sections}, device_id_type=MESH)
        greeted += 1
    pl.semaphore_wait(barrier, greeted)

    def remote(src, dst, send, recv, target):
        return pltpu.make_async_remote_copy(
            src_ref=src, dst_ref=dst, send_sem=send, recv_sem=recv,
            device_id=target, device_id_type=MESH,
        )

    def source(d, which):
        return ((chip - d + chips) % chips) * 2 + which

    def ahead(d, which):
        return ((chip + d) % chips) * 2 + which

    def own_rows(owner):
        return pl.ds(pl.multiple_of(owner * shard, shard), shard)

    def piece(kind, owner, part, k):
        if kind == 0:
            first = (part * QUERY_CUTS + k) * query_size
            return query_w.at[owner, pl.ds(pl.multiple_of(first, 16), query_size)]
        first = pl.multiple_of(owner * shard + part * out_rows, out_rows)
        return out_w.at[pl.ds(first, out_rows), pl.ds(*out_edges[k])]

    def whole(kind, owner):
        if kind == 0:
            return query_w.at[owner]
        return out_w.at[own_rows(owner)]

    def x_copy(kind, d, k, owner):
        ref = piece(kind, owner, g, k)
        return remote(ref, ref, x_send.at[kind, d, k], x_recv.at[kind, d, k], {"seq": ahead(d, core)})

    def y_copy(kind, d, k, e, owner, part):
        ref = piece(kind, owner, part, k)
        return remote(
            ref, ref, y_send.at[kind, d, k, e], y_recv.at[kind, d, k, e], {"groups": (g + e) % groups}
        )

    def d_copy(kind, d, k, e, owner):
        ref = piece(kind, owner, (g - e + groups) % groups, k)
        return remote(ref, ref, d_send.at[kind, d, k, e], d_recv.at[kind, d, k, e], {"seq": partner})

    def own_copy(kind, owner):
        ref = whole(kind, owner)
        return remote(ref, ref, own_send.at[kind], own_recv.at[kind], {"seq": partner})

    step = -(-width // (HOP_CUTS * LANES)) * LANES
    edges = [(c * step, min(step, width - c * step)) for c in range(HOP_CUTS)]

    def z_copy(t, c):
        columns = pl.ds(*edges[c])
        return remote(
            hidden_ref.at[t, :, columns], arrive.at[t, :, columns],
            z_send.at[t, c], z_recv.at[t, c], {"section": (sec + 1) % sections},
        )

    def w_copy(t, off, side):
        columns = pl.ds(side * kv_width, kv_width)
        return remote(
            cache_ref.at[t, pl.ds(rows - keep, keep), columns], window.at[t, off - 1, :, columns],
            w_send.at[t, off - 1, side], w_recv.at[t, off - 1, side], {"seq": (q + off) % seq},
        )

    def ax_copy(t, d, owner):
        ref = gathered.at[t, owner]
        return remote(ref, ref, ax_send.at[t, d], ax_recv.at[t, d], {"seq": ahead(d, core)})

    def ad_copy(t, d, owner):
        ref = gathered.at[t, owner]
        return remote(ref, ref, ad_send.at[t, d], ad_recv.at[t, d], {"seq": partner})

    def rd_copy(t, d):
        return remote(
            outgoing.at[t, d], incoming.at[t, d], rd_send.at[t, d], rd_recv.at[t, d], {"seq": partner}
        )

    def rx_copy(t, d, c):
        columns = pl.ds(*edges[c])
        return remote(
            incoming.at[t, d, :, columns], final.at[t, d, :, columns],
            rx_send.at[t, d, c], rx_recv.at[t, d, c], {"seq": ahead(d, core)},
        )

    def tables(r):
        lane = lax.broadcasted_iota(jnp.int32, (rows, LANES), 1)
        place = lax.broadcasted_iota(jnp.int32, (rows, LANES), 0) + r * rows
        freq = jnp.exp((lane % half).astype(F32) * (-2.0 * math.log(THETA) / HEAD_DIM))
        angles = place.astype(F32) * freq
        at = pl.ds(pl.multiple_of(r * rows, rows), rows)
        cos_tab[at] = jnp.cos(angles)
        sine = jnp.sin(angles)
        sin_tab[at] = jnp.where((lane % HEAD_DIM) < half, -sine, sine)

    def rotate(tile, cosine, sine):
        lane = lax.broadcasted_iota(jnp.int32, tile.shape, 1)
        first_half = (lane % HEAD_DIM) < half
        swapped = jnp.where(
            first_half, pltpu.roll(tile, LANES - half, 1), pltpu.roll(tile, half, 1)
        )
        return tile * cosine + swapped * sine

    def norm(h):
        widened = h.astype(F32)
        scale = lax.rsqrt(jnp.mean(widened * widened, -1, keepdims=True) + EPSILON)
        return (widened * scale * gain_ref[...]).astype(BF16)

    def transpose_out():
        out_load.wait()
        for first in range(0, width, LANES):
            size = min(LANES, width - first)
            out_w[own_rows(q), first:first + size] = out_t[first:first + size, :].T

    def bias_of(r, length, lanes):
        key = lax.broadcasted_iota(jnp.int32, (span, lanes), 0) - WIN
        row = lax.broadcasted_iota(jnp.int32, (span, lanes), 1) % rows
        column = key + r * rows
        allowed = (key <= row) & (row - key < WIN) & (column >= 0)
        allowed = allowed & ((column < length) | (key == row))
        return jnp.where(allowed, F32(0.0), F32(-1e30))

    def sink_row(first, tiles):
        return jnp.concatenate(
            [jnp.full((1, rows), sink_ref[first + 2 * p], F32) for p in range(tiles)], 1
        )

    low = lax.broadcasted_iota(jnp.int32, (span, LANES), 1) < HEAD_DIM
    ones = jnp.ones((16, span), BF16)

    def attention(pairs, twice, values_t, bias, sinks):
        zero = jnp.zeros_like(twice)
        sides = jnp.concatenate([jnp.where(low, twice, zero), jnp.where(low, zero, twice)], 0)
        scores = lax.dot_general(
            sides, jnp.concatenate(pairs, 0), (((1,), (1,)), ((), ())), preferred_element_type=F32
        )
        extended = jnp.concatenate([values_t, ones], 0)
        parts = []
        for b in range(2):
            masked = scores[b * span:(b + 1) * span] + bias
            top = jnp.maximum(jnp.max(masked, 0, keepdims=True), sinks[b])
            expo = jnp.exp(masked - top).astype(BF16)
            summed = jnp.dot(extended, expo, preferred_element_type=F32)
            whole_sum = summed[HEAD_DIM:HEAD_DIM + 1] + jnp.exp(sinks[b] - top)
            parts.append(summed[:HEAD_DIM] * (1.0 / whole_sum))
        return jnp.concatenate(parts, 0).T.astype(BF16)

    def cache_of(t, normed, cosine, sine, send):
        keys = jnp.dot(normed, pair_ref[:, :kv_width], preferred_element_type=F32)
        for p in range(kv_width // LANES):
            tile = slice(p * LANES, (p + 1) * LANES)
            cache_ref[t, :, tile] = rotate(keys[:, tile], cosine, sine).astype(BF16)
        if send:
            for off in range(1, depth + 1):

                @pl.when(q + off < seq)
                def _():
                    w_copy(t, off, 0).start()

        values = jnp.dot(normed, pair_ref[:, kv_width:], preferred_element_type=F32)
        cache_ref[t, :, kv_width:] = values.astype(BF16)
        if send:
            for off in range(1, depth + 1):

                @pl.when(q + off < seq)
                def _():
                    w_copy(t, off, 1).start()

    mine = pl.ds(pl.multiple_of(q * rows, rows), rows)

    def first_section():
        tiles = shard // LANES
        gain_load.wait()
        tokens_load.wait()
        for t in range(micro):
            hbuf[t] = tokens_ref[order_ref[t]]
            gathered[t, q] = norm(hbuf[t])
            if t < micro - 1 or micro < 3:
                for d in range(1, chips):
                    ax_copy(t, d, q).start()
            ad_copy(t, 0, q).start()
        for r in range(seq):
            tables(r)
        kd_buf[:WIN] = jnp.zeros((WIN, LANES), BF16)
        vd_buf[:WIN] = jnp.zeros((WIN, LANES), BF16)
        transpose_out()
        pair_load.wait()
        for j in range(groups):
            for k in range(QUERY_CUTS):
                query_load(j, k).wait()
        for t in range(micro):
            cache_of(t, gathered[t, q], cos_tab[mine], sin_tab[mine], False)

        kv_head = (q * own_heads) // group
        pair_at = pl.ds(pl.multiple_of((kv_head // 2) * LANES, LANES), LANES)
        value_at = pl.ds(pl.multiple_of(kv_width + (kv_head // 2) * LANES, LANES), LANES)
        sinks = [sink_row(q * own_heads + b, tiles) for b in range(2)]

        def double(tile):
            lane = lax.broadcasted_iota(jnp.int32, tile.shape, 1)
            kept = jnp.where(lane // HEAD_DIM == kv_head % 2, tile, 0.0)
            return (kept + pltpu.roll(kept, HEAD_DIM, 1)).astype(BF16)

        def compute(t):
            for d in range(1, chips):
                ax_copy(t, d, source(d, core)).wait_recv()
                ad_copy(t, d, source(d, core)).start()
            for d in range(chips):
                ad_copy(t, d, source(d, 1 - core)).wait_recv()
            length = length_ref[order_ref[t]]
            normed = gathered[t].reshape(total, width)
            cosine, sine = cos_tab[...], sin_tab[...]
            keys = jnp.dot(normed, pair_ref[:, pair_at], preferred_element_type=F32)
            kd_buf[WIN:] = double(rotate(keys, cosine, sine))
            vd_buf[WIN:] = double(jnp.dot(normed, pair_ref[:, value_at], preferred_element_type=F32))
            queries = jnp.dot(normed, query_w[q], preferred_element_type=F32)
            for p in range(tiles):
                tile = slice(p * LANES, (p + 1) * LANES)
                tq[:, tile] = (rotate(queries[:, tile], cosine, sine) * 0.125).astype(BF16)
            for r in range(seq):
                at = slice(r * rows, r * rows + span)
                some = attention(
                    [tq[r * rows:(r + 1) * rows, p * LANES:(p + 1) * LANES] for p in range(tiles)],
                    kd_buf[at], vd_buf[at].T[:HEAD_DIM], bias_of(r, length, tiles * rows), sinks,
                )
                for p in range(tiles):
                    ctx[r, :, p * LANES:(p + 1) * LANES] = some[p * rows:(p + 1) * rows]
            weights = out_w[own_rows(q), :]
            there = jnp.dot(
                jnp.concatenate([ctx[ahead(d, 1 - core)] for d in range(chips)], 0), weights,
                preferred_element_type=F32,
            )
            for d in list(range(1, chips)) + [0]:
                outgoing[t, d] = there[d * rows:(d + 1) * rows].astype(BF16)
                rd_copy(t, d).start()
            here = jnp.dot(
                jnp.concatenate([ctx[ahead(d, core)] for d in range(chips)], 0), weights,
                preferred_element_type=F32,
            )
            acc[t] = hbuf[t].astype(F32) + here[:rows]
            for d in range(1, chips):
                rd_copy(t, d).wait_recv()
                joined = here[d * rows:(d + 1) * rows] + incoming[t, d].astype(F32)
                incoming[t, d] = joined.astype(BF16)
                for c in range(HOP_CUTS):
                    rx_copy(t, d, c).start()

        def finish(t):
            rd_copy(t, 0).wait_recv()
            for c, (first, size) in enumerate(edges):
                columns = slice(first, first + size)
                joined = acc[t, :, columns] + incoming[t, 0, :, columns].astype(F32)
                for d in range(1, chips):
                    rx_copy(t, d, c).wait_recv()
                    joined = joined + final[t, d, :, columns].astype(F32)
                hidden_ref[t, :, columns] = joined.astype(BF16)
                if sections > 1:
                    z_copy(t, c).start()

        @pl.loop(0, micro)
        def _(t):
            if micro >= 3:

                @pl.when(t == micro - 1)
                def _():
                    finish(0)

            compute(t)
            if micro >= 3:

                @pl.when(t == 0)
                def _():
                    for d in range(1, chips):
                        ax_copy(micro - 1, d, q).start()

        @pl.loop(1 if micro >= 3 else 0, micro)
        def _(t):
            finish(t)

        for t in range(micro):
            for d in range(1, chips):
                ax_copy(t, d, q).wait_send()
                for c in range(HOP_CUTS):
                    rx_copy(t, d, c).wait_send()
            for d in range(chips):
                ad_copy(t, d, source(d, core)).wait_send()
                rd_copy(t, d).wait_send()

    def later_section():
        tiles = group // 2
        plan = [(kind, k, d) for kind in range(2) for k in range(cuts[kind]) for d in range(1, chips)]
        for k in range(QUERY_CUTS):
            query_load(0, k).wait()
            for d in range(1, chips):
                x_copy(0, d, k, q).start()
        transpose_out()
        for k in range(cuts[1]):
            for d in range(1, chips):
                x_copy(1, d, k, q).start()
        for j in range(1, groups):
            for k in range(QUERY_CUTS):
                query_load(j, k).wait()
        for kind in range(2):
            own_copy(kind, q).start()
        tables(q)
        for off in range(1, depth + 1):

            @pl.when(q < off)
            def _():
                window[:, off - 1] = jnp.zeros((micro, keep, 2 * kv_width), BF16)

        for h in range(kv_heads):
            for b in range(2):
                sink_rows[2 * h + b:2 * h + b + 1, :] = sink_row(h * group + b, tiles)
        gain_load.wait()
        pair_load.wait()

        def relay_y(kind, k, d):
            for e in range(1, groups):
                y_copy(kind, d, k, e, source(d, core), (g - e + groups) % groups).wait_recv()
                d_copy(kind, d, k, e, source(d, core)).start()

        previous = None
        for kind, k, d in plan:
            x_copy(kind, d, k, source(d, core)).wait_recv()
            for e in range(1, groups):
                y_copy(kind, d, k, e, source(d, core), g).start()
            d_copy(kind, d, k, 0, source(d, core)).start()
            if previous is not None:
                relay_y(*previous)
            previous = (kind, k, d)
        if previous is not None:
            relay_y(*previous)
        for kind in range(2):
            own_copy(kind, partner).wait_recv()
        for kind, k, d in plan:
            for e in range(groups):
                d_copy(kind, d, k, e, source(d, 1 - core)).wait_recv()

        def enter(t):
            for c in range(HOP_CUTS):
                z_copy(t, c).wait_recv()
            normed_ref[t] = norm(arrive[t])
            cache_of(t, normed_ref[t], cos_tab[mine], sin_tab[mine], True)

        def attend(t):
            length = length_ref[order_ref[t]]
            normed = normed_ref[t]
            cosine, sine = cos_tab[mine], sin_tab[mine]
            for s in range(seq):
                queries = jnp.dot(normed, query_w[s], preferred_element_type=F32)
                for p in range(shard // LANES):
                    rotated = rotate(queries[:, p * LANES:(p + 1) * LANES], cosine, sine) * 0.125
                    qbuf[:, s * shard + p * LANES:s * shard + (p + 1) * LANES] = rotated.astype(BF16)
            for off in range(1, depth + 1):

                @pl.when(q >= off)
                def _():
                    w_copy(t, off, 0).wait_recv()
                    w_copy(t, off, 1).wait_recv()

            bias = bias_of(q, length, tiles * rows)

            def span_of(first, size):
                at = slice(first, first + size)
                parts = [window[t, off - 1, :, at] for off in range(depth, 0, -1)]
                return jnp.concatenate(parts + [cache_ref[t, :, at]], 0)

            for pair in range(kv_heads // 2):
                values_t = span_of(kv_width + pair * LANES, LANES).T
                for e in range(2):
                    h = pair * 2 + e
                    head = span_of(h * HEAD_DIM, HEAD_DIM)
                    at = [(h * tiles + p) * LANES for p in range(tiles)]
                    some = attention(
                        [qbuf[:, a:a + LANES] for a in at], jnp.concatenate([head, head], 1),
                        values_t[e * HEAD_DIM:(e + 1) * HEAD_DIM], bias,
                        [sink_rows[2 * h + b:2 * h + b + 1, :] for b in range(2)],
                    )
                    for p in range(tiles):
                        cbuf[:, at[p]:at[p] + LANES] = some[p * rows:(p + 1) * rows]

        def slot(t, carry):
            enter(t)
            attend(t)
            for c, (first, size) in enumerate(edges):
                columns = slice(first, first + size)
                output = jnp.dot(cbuf[...], out_w[:, columns], preferred_element_type=F32)
                hidden_ref[t, :, columns] = (arrive[t, :, columns].astype(F32) + output).astype(BF16)

                @pl.when(sec + 1 < sections)
                def _():
                    z_copy(t, c).start()

            return carry

        lax.fori_loop(0, micro, slot, 0)

        for kind, k, d in plan:
            x_copy(kind, d, k, q).wait_send()
            for e in range(1, groups):
                y_copy(kind, d, k, e, source(d, core), g).wait_send()
            for e in range(groups):
                d_copy(kind, d, k, e, source(d, core)).wait_send()
        for kind in range(2):
            own_copy(kind, q).wait_send()
        for t in range(micro):
            for off in range(1, depth + 1):

                @pl.when(q + off < seq)
                def _():
                    w_copy(t, off, 0).wait_send()
                    w_copy(t, off, 1).wait_send()


    @pl.when(sec == 0)
    def _():
        first_section()

    @pl.when(sec > 0)
    def _():
        later_section()

    @pl.when(sec + 1 < sections)
    def _():
        for t in range(micro):
            for c in range(HOP_CUTS):
                z_copy(t, c).wait_send()


def per_device(
    shape,
    tokens, block_order, prompt_lengths, norm_gain, w_query, w_key_value, w_out, sink_logits
):
    groups, sections, seq = shape
    micro, rows, width = tokens.shape
    shard = w_query.shape[2]
    pair_width = w_key_value.shape[2]
    kv_heads = pair_width // 2 // HEAD_DIM
    lanes = seq * shard // (pair_width // 2) // 2 * rows
    chips = seq // 2
    keep = min(WIN, rows)
    depth = WIN // keep
    most = max(QUERY_CUTS, -(-width // OUT_STEP))
    limit = (52 if seq * rows <= 512 else 57) * 1024 * 1024
    dma = pltpu.SemaphoreType.DMA
    vmem = pl.BlockSpec(memory_space=pltpu.VMEM)
    smem = pl.BlockSpec(memory_space=pltpu.SMEM)
    hbm = pl.BlockSpec(memory_space=pltpu.HBM)
    hidden, cache = pl.pallas_call(
        functools.partial(kernel, shape),
        out_shape=(
            jax.ShapeDtypeStruct((micro, rows, width), BF16),
            jax.ShapeDtypeStruct((micro, rows, pair_width), BF16),
        ),
        in_specs=[smem] * 3 + [hbm] * 5,
        out_specs=(vmem, vmem),
        scratch_shapes=[
            pltpu.VMEM((micro, rows, width), BF16),
            pltpu.VMEM((1, width), F32),
            pltpu.VMEM((width, pair_width), BF16),
            pltpu.VMEM((width, shard), BF16),
            pltpu.VMEM((seq * rows, LANES), F32),
            pltpu.VMEM((seq * rows, LANES), F32),
            pltpu.VMEM((seq, width, shard), BF16),
            pltpu.VMEM((seq * shard, width), BF16),
            pltpu.VMEM((micro, rows, width), BF16),
            pltpu.VMEM((micro, depth, keep, pair_width), BF16),
            pltpu.VMEM((micro, rows, width), BF16),
            pltpu.VMEM((micro, rows, width), BF16),
            pltpu.VMEM((rows, seq * shard), BF16),
            pltpu.VMEM((rows, seq * shard), BF16),
            pltpu.VMEM((2 * kv_heads, lanes), F32),
            pltpu.VMEM((micro, seq, rows, width), BF16),
            pltpu.VMEM((seq * rows, shard), BF16),
            pltpu.VMEM((WIN + seq * rows, LANES), BF16),
            pltpu.VMEM((WIN + seq * rows, LANES), BF16),
            pltpu.VMEM((seq, rows, shard), BF16),
            pltpu.VMEM((micro, chips, rows, width), BF16),
            pltpu.VMEM((micro, chips, rows, width), BF16),
            pltpu.VMEM((micro, chips, rows, width), BF16),
            pltpu.VMEM((micro, rows, width), F32),
            dma((groups * QUERY_CUTS + 4,)),
            dma((2, chips, most)),
            dma((2, chips, most)),
            dma((2, chips, most, groups)),
            dma((2, chips, most, groups)),
            dma((2, chips, most, groups)),
            dma((2, chips, most, groups)),
            dma((2,)),
            dma((2,)),
            dma((micro, depth, 2)),
            dma((micro, depth, 2)),
            dma((micro, HOP_CUTS)),
            dma((micro, HOP_CUTS)),
            dma((micro, chips)),
            dma((micro, chips)),
            dma((micro, chips)),
            dma((micro, chips)),
            dma((micro, chips)),
            dma((micro, chips)),
            dma((micro, chips, HOP_CUTS)),
            dma((micro, chips, HOP_CUTS)),
        ],
        compiler_params=pltpu.CompilerParams(
            collective_id=0, has_side_effects=True, vmem_limit_bytes=limit
        ),
    )(
        block_order, prompt_lengths, sink_logits[0],
        tokens, norm_gain, w_key_value[0], w_query[0], w_out[0].T,
    )
    return hidden[None], cache[None]


def solution(mesh):
    in_specs = (
        P("groups", "seq", None),
        P("groups"),
        P("groups"),
        P("section", None),
        P("section", None, "seq"),
        P("section", None, None),
        P("section", "seq", None),
        P("section", None),
    )
    out_specs = (P("section", "groups", "seq", None), P("section", "groups", "seq", None))
    shape = tuple(mesh.shape[name] for name in ("groups", "section", "seq"))
    return jax.shard_map(
        functools.partial(per_device, shape),
        mesh=mesh, in_specs=in_specs, out_specs=out_specs, check_vma=False,
    )
```

```python
import functools
import math

import jax
import jax.numpy as jnp
from jax import lax
from jax.experimental import pallas as pl
from jax.experimental.pallas import tpu as pltpu
from jax.sharding import PartitionSpec as P

HEAD_DIM = 64
WIN = 128
LANES = 128
THETA = 150000.0
EPSILON = 1e-05
MESH = pl.DeviceIdType.MESH
F32 = jnp.float32
BF16 = jnp.bfloat16
QUERY_CUTS = 5
OUT_STEP = 256
HOP_CUTS = 3
SECOND_ORDER = "e0 f q0 r f r f f a0 w0 o00 r e1 r q1 w1 o01 r f w2 o02 a1 o10 o11 o12"
AHEAD = 2


def out_pieces(width):
    direct = width % LANES + LANES
    coarse = (width - direct) // OUT_STEP * OUT_STEP
    edges = [(c, OUT_STEP) for c in range(0, coarse - OUT_STEP, OUT_STEP)]
    edges += [(c, LANES) for c in range(coarse - OUT_STEP, width - direct, LANES)]
    return edges + [(width - direct, direct)]


def kernel(
    shape,
    whole_ref, real_ref, real_row,
    tokens_hbm, pair_hbm, query_hbm, out_hbm,
    hidden_ref, cache_ref,
    tokens_ref, pair_ref, out_t, cos_tab, sin_tab,
    query_w, out_w, arrive, window, hbuf, normed_ref, qbuf, cbuf, sink_rows,
    gathered, tq, kd_buf, vd_buf, ctx, outgoing, incoming, final, acc,
    local_sem, x_send, x_recv, y_send, y_recv, d_send, d_recv, own_send, own_recv,
    w_send, w_recv, z_send, z_recv,
    ax_send, ax_recv, ad_send, ad_recv, rd_send, rd_recv, rx_send, rx_recv,
):
    groups, sections, seq = shape
    chips = seq // 2
    g = lax.axis_index("groups")
    sec = lax.axis_index("section")
    q = lax.axis_index("seq")
    chip, core = q // 2, q % 2
    partner = chip * 2 + (1 - core)
    micro, rows, width = hidden_ref.shape
    shard = query_w.shape[2]
    heads_width = seq * shard
    kv_width = pair_ref.shape[1] // 2
    kv_heads = kv_width // HEAD_DIM
    group = heads_width // kv_width
    keep = min(WIN, rows)
    depth = WIN // keep
    span = WIN + rows
    total = seq * rows
    half = HEAD_DIM // 2
    own_heads = shard // HEAD_DIM

    query_size = width // groups // QUERY_CUTS
    out_rows = shard // groups
    out_edges = out_pieces(width)
    last_edge = out_edges[-1]
    cuts = (QUERY_CUTS, len(out_edges) - 1, 1)

    def query_load(j, k):
        first = pl.multiple_of((((g + j) % groups) * QUERY_CUTS + k) * query_size, 16)
        return pltpu.make_async_copy(
            query_hbm.at[pl.ds(first, query_size)], query_w.at[q, pl.ds(first, query_size)],
            local_sem.at[j * QUERY_CUTS + k],
        )

    base = groups * QUERY_CUTS
    out_load = pltpu.make_async_copy(out_hbm, out_t, local_sem.at[base])
    pair_load = pltpu.make_async_copy(pair_hbm, pair_ref, local_sem.at[base + 1])
    tokens_load = pltpu.make_async_copy(tokens_hbm, tokens_ref, local_sem.at[base + 2])

    @pl.when(sec == 0)
    def _():
        tokens_load.start()

    for j in range(groups):
        for k in range(QUERY_CUTS):
            query_load(j, k).start()
    out_load.start()
    pair_load.start()

    barrier = pltpu.get_barrier_semaphore()
    greeted = 0
    for d in range(1, seq):
        pl.semaphore_signal(barrier, 1, device_id={"seq": (q + d) % seq}, device_id_type=MESH)
        greeted += 1
    for e in range(1, groups):
        pl.semaphore_signal(barrier, 1, device_id={"groups": (g + e) % groups}, device_id_type=MESH)
        greeted += 1
    for s in sorted({1 % sections, (sections - 1) % sections} - {0}):
        pl.semaphore_signal(barrier, 1, device_id={"section": (sec + s) % sections}, device_id_type=MESH)
        greeted += 1
    pl.semaphore_wait(barrier, greeted)

    def remote(src, dst, send, recv, target):
        return pltpu.make_async_remote_copy(
            src_ref=src, dst_ref=dst, send_sem=send, recv_sem=recv,
            device_id=target, device_id_type=MESH,
        )

    def source(d, which):
        return ((chip - d + chips) % chips) * 2 + which

    def ahead(d, which):
        return ((chip + d) % chips) * 2 + which

    def own_rows(owner):
        return pl.ds(pl.multiple_of(owner * shard, shard), shard)

    def piece(kind, owner, part, k):
        if kind == 0:
            first = (part * QUERY_CUTS + k) * query_size
            return query_w.at[owner, pl.ds(pl.multiple_of(first, 16), query_size)]
        if kind == 2:
            return out_w.at[own_rows(owner), pl.ds(*last_edge)]
        first = pl.multiple_of(owner * shard + part * out_rows, out_rows)
        return out_w.at[pl.ds(first, out_rows), pl.ds(*out_edges[k])]

    def whole(kind, owner):
        if kind == 0:
            return query_w.at[owner]
        return out_w.at[own_rows(owner)]

    slots = (0, cuts[0], cuts[0] + cuts[1])

    def x_copy(kind, d, k, owner):
        ref = piece(kind, owner, g, k)
        return remote(ref, ref, x_send.at[kind, d - 1], x_recv.at[d - 1, slots[kind] + k], {"seq": ahead(d, core)})

    def y_copy(kind, d, k, e, owner, part):
        ref = piece(kind, owner, part, k)
        return remote(
            ref, ref, y_send.at[kind, d - 1, e - 1], y_recv.at[d - 1, slots[kind] + k, e - 1], {"groups": (g + e) % groups}
        )

    def d_copy(kind, d, k, e, owner):
        ref = piece(kind, owner, (g - e + groups) % groups, k)
        return remote(ref, ref, d_send.at[kind], d_recv.at[0 if kind == 0 else slots[kind] - slots[1] + 1 + k], {"seq": partner})

    def part_of(kind, owner, part):
        if kind == 0:
            size = QUERY_CUTS * query_size
            return query_w.at[owner, pl.ds(pl.multiple_of(part * size, 16), size)]
        if kind == 2:
            return piece(2, owner, part, 0)
        first = pl.multiple_of(owner * shard + part * out_rows, out_rows)
        return out_w.at[pl.ds(first, out_rows), pl.ds(0, last_edge[0])]

    def sent(ref, sem):
        remote(ref, ref, sem, sem, {"seq": partner}).wait_send()

    def landed(ref, sem):
        remote(ref, ref, sem, sem, {"seq": partner}).wait_recv()

    def own_copy(kind, owner):
        ref = whole(kind, owner)
        return remote(ref, ref, own_send.at[kind], own_recv.at[kind], {"seq": partner})

    step = -(-width // (HOP_CUTS * LANES)) * LANES
    edges = [(c * step, min(step, width - c * step)) for c in range(HOP_CUTS)]

    def z_copy(t, c):
        columns = pl.ds(*edges[c])
        return remote(
            hidden_ref.at[t, :, columns], arrive.at[t, :, columns],
            z_send.at[0], z_recv.at[t], {"section": (sec + 1) % sections},
        )

    def w_copy(t, off):
        return remote(
            cache_ref.at[t, pl.ds(rows - keep, keep)], window.at[t, off - 1],
            w_send.at[off - 1], w_recv.at[t, off - 1], {"seq": (q + off) % seq},
        )

    def ax_copy(t, d, owner):
        ref = gathered.at[t, owner]
        return remote(ref, ref, ax_send.at[d - 1], ax_recv.at[t, d - 1], {"seq": ahead(d, core)})

    def ad_copy(t, d, owner):
        ref = gathered.at[t, owner]
        return remote(ref, ref, ad_send.at[0], ad_recv.at[t], {"seq": partner})

    def rd_copy(t, d):
        return remote(
            outgoing.at[t, d], incoming.at[t, d], rd_send.at[0], rd_recv.at[t, d], {"seq": partner}
        )

    def rx_copy(t, d, c):
        columns = pl.ds(*edges[c])
        return remote(
            incoming.at[t, d, :, columns], final.at[t, d, :, columns],
            rx_send.at[d - 1], rx_recv.at[t, d - 1, c], {"seq": ahead(d, core)},
        )

    def tables(r):
        lane = lax.broadcasted_iota(jnp.int32, (rows, LANES), 1)
        place = lax.broadcasted_iota(jnp.int32, (rows, LANES), 0) + r * rows
        freq = jnp.exp((lane % half).astype(F32) * (-2.0 * math.log(THETA) / HEAD_DIM))
        angles = place.astype(F32) * freq
        at = pl.ds(pl.multiple_of(r * rows, rows), rows)
        cos_tab[at] = jnp.cos(angles)
        sine = jnp.sin(angles)
        sin_tab[at] = jnp.where((lane % HEAD_DIM) < half, -sine, sine)

    def rotate(tile, cosine, sine):
        lane = lax.broadcasted_iota(jnp.int32, tile.shape, 1)
        first_half = (lane % HEAD_DIM) < half
        swapped = jnp.where(
            first_half, pltpu.roll(tile, LANES - half, 1), pltpu.roll(tile, half, 1)
        )
        return tile * cosine + swapped * sine

    def norm(h):
        widened = h.astype(F32)
        scale = lax.rsqrt(jnp.mean(widened * widened, -1, keepdims=True) + EPSILON)
        return (widened * scale * real_row[:, :width]).astype(BF16)

    def transpose_out():
        out_load.wait()
        for first in range(0, width, LANES):
            size = min(LANES, width - first)
            out_w[own_rows(q), first:first + size] = out_t[first:first + size, :].T

    def bias_of(r, length, lanes):
        key = lax.broadcasted_iota(jnp.int32, (span, lanes), 0) - WIN
        row = lax.broadcasted_iota(jnp.int32, (span, lanes), 1) % rows
        column = key + r * rows
        allowed = (key <= row) & (row - key < WIN) & (column >= 0)
        allowed = allowed & ((column < length) | (key == row))
        return jnp.where(allowed, F32(0.0), F32(-1e30))

    def sink_row(first, tiles):
        return jnp.concatenate(
            [jnp.full((1, rows), real_ref[0, width + first + 2 * p], F32) for p in range(tiles)], 1
        )

    low = lax.broadcasted_iota(jnp.int32, (span, LANES), 1) < HEAD_DIM
    ones = jnp.ones((16, span), BF16)

    def attention(pairs, twice, values_t, bias, sinks):
        zero = jnp.zeros_like(twice)
        sides = jnp.concatenate([jnp.where(low, twice, zero), jnp.where(low, zero, twice)], 0)
        scores = lax.dot_general(
            sides, jnp.concatenate(pairs, 0), (((1,), (1,)), ((), ())), preferred_element_type=F32
        )
        extended = jnp.concatenate([values_t, ones], 0)
        parts = []
        for b in range(2):
            masked = scores[b * span:(b + 1) * span] + bias
            top = jnp.maximum(jnp.max(masked, 0, keepdims=True), sinks[b])
            expo = jnp.exp(masked - top).astype(BF16)
            summed = jnp.dot(extended, expo, preferred_element_type=F32)
            whole_sum = summed[HEAD_DIM:HEAD_DIM + 1] + jnp.exp(sinks[b] - top)
            parts.append(summed[:HEAD_DIM] * (1.0 / whole_sum))
        return jnp.concatenate(parts, 0).T.astype(BF16)

    def cache_of(t, normed, cosine, sine, send):
        keys = jnp.dot(normed, pair_ref[:, :kv_width], preferred_element_type=F32)
        for p in range(kv_width // LANES):
            tile = slice(p * LANES, (p + 1) * LANES)
            cache_ref[t, :, tile] = rotate(keys[:, tile], cosine, sine).astype(BF16)
        values = jnp.dot(normed, pair_ref[:, kv_width:], preferred_element_type=F32)
        cache_ref[t, :, kv_width:] = values.astype(BF16)
        if send:
            for off in range(1, depth + 1):

                @pl.when(q + off < seq)
                def _():
                    w_copy(t, off).start()

    mine = pl.ds(pl.multiple_of(q * rows, rows), rows)

    def first_section():
        tiles = shard // LANES
        tokens_load.wait()
        for t in range(micro):
            hbuf[t] = tokens_ref[whole_ref[t]]
            gathered[t, q] = norm(hbuf[t])
            if t < micro - 1 or micro < 3:
                for d in range(1, chips):
                    ax_copy(t, d, q).start()
            ad_copy(t, 0, q).start()
        for r in range(seq):
            tables(r)
        kd_buf[:WIN] = jnp.zeros((WIN, LANES), BF16)
        vd_buf[:WIN] = jnp.zeros((WIN, LANES), BF16)
        transpose_out()
        pair_load.wait()
        for j in range(groups):
            for k in range(QUERY_CUTS):
                query_load(j, k).wait()
        for t in range(micro):
            cache_of(t, gathered[t, q], cos_tab[mine], sin_tab[mine], False)

        kv_head = (q * own_heads) // group
        pair_at = pl.ds(pl.multiple_of((kv_head // 2) * LANES, LANES), LANES)
        value_at = pl.ds(pl.multiple_of(kv_width + (kv_head // 2) * LANES, LANES), LANES)
        sinks = [sink_row(q * own_heads + b, tiles) for b in range(2)]

        def double(tile):
            lane = lax.broadcasted_iota(jnp.int32, tile.shape, 1)
            kept = jnp.where(lane // HEAD_DIM == kv_head % 2, tile, 0.0)
            return (kept + pltpu.roll(kept, HEAD_DIM, 1)).astype(BF16)

        def finish(t):
            rd_copy(t, 0).wait_recv()
            for c, (first, size) in enumerate(edges):
                columns = slice(first, first + size)
                joined = acc[t, :, columns] + incoming[t, 0, :, columns].astype(F32)
                for d in range(1, chips):
                    rx_copy(t, d, c).wait_recv()
                    joined = joined + final[t, d, :, columns].astype(F32)
                hidden_ref[t, :, columns] = joined.astype(BF16)
                if sections > 1:
                    z_copy(t, c).start()

        def compute(t):
            for d in range(1, chips):
                ax_copy(t, d, source(d, core)).wait_recv()
                ad_copy(t, d, source(d, core)).start()
            landed(outgoing.at[t], ad_recv.at[t])
            length = whole_ref[micro + whole_ref[t]]
            normed = gathered[t].reshape(total, width)
            cosine, sine = cos_tab[...], sin_tab[...]
            keys = jnp.dot(normed, pair_ref[:, pair_at], preferred_element_type=F32)
            kd_buf[WIN:] = double(rotate(keys, cosine, sine))
            vd_buf[WIN:] = double(jnp.dot(normed, pair_ref[:, value_at], preferred_element_type=F32))
            queries = jnp.dot(normed, query_w[q], preferred_element_type=F32)
            for p in range(tiles):
                tile = slice(p * LANES, (p + 1) * LANES)
                tq[:, tile] = (rotate(queries[:, tile], cosine, sine) * 0.125).astype(BF16)
            for r in range(seq):
                at = slice(r * rows, r * rows + span)
                some = attention(
                    [tq[r * rows:(r + 1) * rows, p * LANES:(p + 1) * LANES] for p in range(tiles)],
                    kd_buf[at], vd_buf[at].T[:HEAD_DIM], bias_of(r, length, tiles * rows), sinks,
                )
                for p in range(tiles):
                    ctx[r, :, p * LANES:(p + 1) * LANES] = some[p * rows:(p + 1) * rows]
            if micro >= 3:

                @pl.when(t == micro - 1)
                def _():
                    finish(1)

            weights = out_w[own_rows(q), :]
            there = jnp.dot(
                jnp.concatenate([ctx[ahead(d, 1 - core)] for d in range(chips)], 0), weights,
                preferred_element_type=F32,
            )
            for d in list(range(1, chips)) + [0]:
                outgoing[t, d] = there[d * rows:(d + 1) * rows].astype(BF16)
                rd_copy(t, d).start()
            here = jnp.dot(
                jnp.concatenate([ctx[ahead(d, core)] for d in range(chips)], 0), weights,
                preferred_element_type=F32,
            )
            acc[t] = hbuf[t].astype(F32) + here[:rows]
            for d in range(1, chips):
                rd_copy(t, d).wait_recv()
                joined = here[d * rows:(d + 1) * rows] + incoming[t, d].astype(F32)
                incoming[t, d] = joined.astype(BF16)
                for c in range(HOP_CUTS):
                    rx_copy(t, d, c).start()

        @pl.loop(0, micro)
        def _(t):
            if micro >= 3:

                @pl.when(t == 2)
                def _():
                    finish(0)

            compute(t)
            if micro >= 3:

                @pl.when(t == 0)
                def _():
                    for d in range(1, chips):
                        ax_copy(micro - 1, d, q).start()

        @pl.loop(2 if micro >= 3 else 0, micro)
        def _(t):
            finish(t)

        for d in range(1, chips):
            sent(gathered.at[:, q], ax_send.at[d - 1])
            sent(incoming.at[:, d], rx_send.at[d - 1])
        sent(outgoing, ad_send.at[0])
        sent(outgoing, rd_send.at[0])

    def later_section():
        tiles = group // 2
        for k in range(QUERY_CUTS):
            query_load(0, k).wait()
            for d in range(1, chips):
                x_copy(0, d, k, q).start()
        transpose_out()
        rounds = [(kind, k) for kind in range(3) for k in range(cuts[kind])]
        outs = rounds[cuts[0]:]

        def send_out(one):
            for d in range(1, chips):
                x_copy(one[0], d, one[1], q).start()

        for one in outs[:AHEAD]:
            send_out(one)

        @pl.when(sec > 1)
        def _():
            for one in outs[AHEAD:]:
                send_out(one)

        for j in range(1, groups):
            for k in range(QUERY_CUTS):
                query_load(j, k).wait()
        for kind in range(2):
            own_copy(kind, q).start()
        tables(q)
        for off in range(1, depth + 1):

            @pl.when(q < off)
            def _():
                window[:, off - 1] = jnp.zeros((micro, keep, 2 * kv_width), BF16)

        for h in range(kv_heads):
            for b in range(2):
                sink_rows[2 * h + b:2 * h + b + 1, :] = sink_row(h * group + b, tiles)
        pair_load.wait()

        def forward(kind, k):
            for d in range(1, chips):
                x_copy(kind, d, k, source(d, core)).wait_recv()
                if kind < 2:
                    for e in range(1, groups):
                        y_copy(kind, d, k, e, source(d, core), g).start()
                d_copy(kind, d, k, 0, source(d, core)).start()

        def relay(kind, k):
            if kind < 2:
                for d in range(1, chips):
                    for e in range(1, groups):
                        y_copy(kind, d, k, e, source(d, core), (g - e + groups) % groups).wait_recv()
                        d_copy(kind, d, k, e, source(d, core)).start()

        def several(first, size):
            return out_w.at[pl.ds(0, (chips - 1) * shard), pl.ds(first, size)]

        def ready_queries():
            own_copy(0, partner).wait_recv()
            if chips > 1:
                landed(query_w.at[pl.ds(0, chips - 1)], d_recv.at[0])

        def ready(k):
            if k == 0:
                own_copy(1, partner).wait_recv()
            if chips > 1:
                landed(several(*out_edges[k]), d_recv.at[1 + k])

        def gather_sent():
            for kind in range(3):
                for d in range(1, chips):
                    sent(part_of(kind, q, g), x_send.at[kind, d - 1])
                    for e in range(1, groups if kind < 2 else 1):
                        sent(part_of(kind, source(d, core), g), y_send.at[kind, d - 1, e - 1])
            if chips > 1:
                sent(query_w.at[pl.ds(0, chips - 1)], d_send.at[0])
                sent(several(0, last_edge[0]), d_send.at[1])
                sent(several(*last_edge), d_send.at[2])
            for kind in range(2):
                own_copy(kind, q).wait_send()

        def enter(t):
            landed(arrive.at[t], z_recv.at[t])
            normed_ref[t] = norm(arrive[t])
            cache_of(t, normed_ref[t], cos_tab[mine], sin_tab[mine], True)

        def ask(t):
            normed = normed_ref[t]
            cosine, sine = cos_tab[mine], sin_tab[mine]
            for s in range(seq):
                queries = jnp.dot(normed, query_w[s], preferred_element_type=F32)
                for p in range(shard // LANES):
                    rotated = rotate(queries[:, p * LANES:(p + 1) * LANES], cosine, sine) * 0.125
                    qbuf[:, s * shard + p * LANES:s * shard + (p + 1) * LANES] = rotated.astype(BF16)

        def attend(t):
            length = whole_ref[micro + whole_ref[t]]
            for off in range(1, depth + 1):

                @pl.when(q >= off)
                def _():
                    landed(window.at[t, off - 1], w_recv.at[t, off - 1])

            bias = bias_of(q, length, tiles * rows)

            def span_of(first, size):
                at = slice(first, first + size)
                parts = [window[t, off - 1, :, at] for off in range(depth, 0, -1)]
                return jnp.concatenate(parts + [cache_ref[t, :, at]], 0)

            for pair in range(kv_heads // 2):
                values_t = span_of(kv_width + pair * LANES, LANES).T
                for e in range(2):
                    h = pair * 2 + e
                    head = span_of(h * HEAD_DIM, HEAD_DIM)
                    at = [(h * tiles + p) * LANES for p in range(tiles)]
                    some = attention(
                        [qbuf[:, a:a + LANES] for a in at], jnp.concatenate([head, head], 1),
                        values_t[e * HEAD_DIM:(e + 1) * HEAD_DIM], bias,
                        [sink_rows[2 * h + b:2 * h + b + 1, :] for b in range(2)],
                    )
                    for p in range(tiles):
                        cbuf[t, :, at[p]:at[p] + LANES] = some[p * rows:(p + 1) * rows]

        def leave(t, c, send=True):
            first, size = edges[c]
            columns = slice(first, first + size)
            output = jnp.dot(cbuf[t], out_w[:, columns], preferred_element_type=F32)
            hidden_ref[t, :, columns] = (arrive[t, :, columns].astype(F32) + output).astype(BF16)
            if send:
                z_copy(t, c).start()

        needed = [[] for c in range(HOP_CUTS)]
        for k, (first, size) in enumerate(out_edges):
            needed[first // step].append(k)

        @pl.when(sec == 1)
        def _():
            waiting, relayed = list(rounds), []

            def forward_next():
                if waiting:
                    one = waiting.pop(0)
                    forward(*one)
                    at = rounds.index(one) + AHEAD
                    if one[0] and at < len(rounds):
                        send_out(rounds[at])
                    relayed.append(one)

            def relay_next():
                if relayed:
                    relay(*relayed.pop(0))

            while len(waiting) > len(outs) - 2:
                forward_next()
                if len(relayed) > 1:
                    relay_next()
            while relayed and relayed[0][0] == 0:
                relay_next()
            ready_queries()
            for what in SECOND_ORDER.split():
                if what[0] == "f":
                    forward_next()
                elif what[0] == "r":
                    relay_next()
                elif what[0] == "w":
                    for k in needed[int(what[1])]:
                        ready(k)
                elif what[0] == "o":
                    leave(int(what[1]), int(what[2]), False)

                    @pl.when(sec + 1 < sections)
                    def _():
                        z_copy(int(what[1]), int(what[2])).start()

                else:
                    (enter, ask, attend)["eqa".index(what[0])](int(what[1]))

        @pl.when(sec > 1)
        def _():
            previous = None
            for one in rounds:
                forward(*one)
                if previous is not None:
                    relay(*previous)
                previous = one
            relay(*previous)
            ready_queries()
            for k in range(len(out_edges)):
                ready(k)
            gather_sent()

        def slot(send, t, carry):
            enter(t)
            ask(t)
            attend(t)
            for c in range(HOP_CUTS):
                leave(t, c, send)
            return carry

        start = jnp.where(sec == 1, 2, 0)

        @pl.when(sec + 1 < sections)
        def _():
            lax.fori_loop(start, micro, functools.partial(slot, True), 0)

        @pl.when(sec + 1 == sections)
        def _():
            lax.fori_loop(start, micro, functools.partial(slot, False), 0)

        @pl.when(sec == 1)
        def _():
            gather_sent()

        for off in range(1, depth + 1):

            @pl.when(q + off < seq)
            def _():
                sent(window.at[:, off - 1], w_send.at[off - 1])

    @pl.when(sec == 0)
    def _():
        first_section()

    @pl.when(sec > 0)
    def _():
        later_section()

    @pl.when(sec + 1 < sections)
    def _():
        sent(arrive, z_send.at[0])


def per_device(
    shape,
    tokens, block_order, prompt_lengths, norm_gain, w_query, w_key_value, w_out, sink_logits
):
    groups, sections, seq = shape
    micro, rows, width = tokens.shape
    shard = w_query.shape[2]
    pair_width = w_key_value.shape[2]
    kv_heads = pair_width // 2 // HEAD_DIM
    lanes = seq * shard // (pair_width // 2) // 2 * rows
    chips = seq // 2
    keep = min(WIN, rows)
    depth = WIN // keep
    others, peers = max(1, chips - 1), max(1, groups - 1)
    rounds = QUERY_CUTS + len(out_pieces(width))
    limit = 55488512 if seq * rows <= 512 else 57 * 1024 * 1024
    real = jnp.concatenate([norm_gain, sink_logits], 1)
    dma = pltpu.SemaphoreType.DMA
    vmem = pl.BlockSpec(memory_space=pltpu.VMEM)
    smem = pl.BlockSpec(memory_space=pltpu.SMEM)
    hbm = pl.BlockSpec(memory_space=pltpu.HBM)
    hidden, cache = pl.pallas_call(
        functools.partial(kernel, shape),
        out_shape=(
            jax.ShapeDtypeStruct((micro, rows, width), BF16),
            jax.ShapeDtypeStruct((micro, rows, pair_width), BF16),
        ),
        in_specs=[smem, smem, vmem] + [hbm] * 4,
        out_specs=(vmem, vmem),
        scratch_shapes=[
            pltpu.VMEM((micro, rows, width), BF16),
            pltpu.VMEM((width, pair_width), BF16),
            pltpu.VMEM((width, shard), BF16),
            pltpu.VMEM((seq * rows, LANES), F32),
            pltpu.VMEM((seq * rows, LANES), F32),
            pltpu.VMEM((seq, width, shard), BF16),
            pltpu.VMEM((seq * shard, width), BF16),
            pltpu.VMEM((micro, rows, width), BF16),
            pltpu.VMEM((micro, depth, keep, pair_width), BF16),
            pltpu.VMEM((micro, rows, width), BF16),
            pltpu.VMEM((micro, rows, width), BF16),
            pltpu.VMEM((rows, seq * shard), BF16),
            pltpu.VMEM((micro, rows, seq * shard), BF16),
            pltpu.VMEM((2 * kv_heads, lanes), F32),
            pltpu.VMEM((micro, seq, rows, width), BF16),
            pltpu.VMEM((seq * rows, shard), BF16),
            pltpu.VMEM((WIN + seq * rows, LANES), BF16),
            pltpu.VMEM((WIN + seq * rows, LANES), BF16),
            pltpu.VMEM((seq, rows, shard), BF16),
            pltpu.VMEM((micro, chips, rows, width), BF16),
            pltpu.VMEM((micro, chips, rows, width), BF16),
            pltpu.VMEM((micro, chips, rows, width), BF16),
            pltpu.VMEM((micro, rows, width), F32),
            dma((groups * QUERY_CUTS + 3,)),
            dma((3, others)),
            dma((others, rounds)),
            dma((3, others, peers)),
            dma((others, rounds, peers)),
            dma((3,)),
            dma((rounds,)),
            dma((2,)),
            dma((2,)),
            dma((depth,)),
            dma((micro, depth)),
            dma((1,)),
            dma((micro,)),
            dma((others,)),
            dma((micro, others)),
            dma((1,)),
            dma((micro,)),
            dma((1,)),
            dma((micro, chips)),
            dma((others,)),
            dma((micro, others, HOP_CUTS)),
        ],
        compiler_params=pltpu.CompilerParams(
            collective_id=0, has_side_effects=True, vmem_limit_bytes=limit
        ),
    )(
        jnp.concatenate([block_order, prompt_lengths]), real, real,
        tokens, w_key_value[0], w_query[0], w_out[0].T,
    )
    return hidden[None], cache[None]


def solution(mesh):
    in_specs = (
        P("groups", "seq", None),
        P("groups"),
        P("groups"),
        P("section", None),
        P("section", None, "seq"),
        P("section", None, None),
        P("section", "seq", None),
        P("section", None),
    )
    out_specs = (P("section", "groups", "seq", None), P("section", "groups", "seq", None))
    shape = tuple(mesh.shape[name] for name in ("groups", "section", "seq"))
    return jax.shard_map(
        functools.partial(per_device, shape),
        mesh=mesh, in_specs=in_specs, out_specs=out_specs, check_vma=False,
    )
```

```python
import functools
import math

import jax
import jax.numpy as jnp
from jax import lax
from jax.experimental import pallas as pl
from jax.experimental.pallas import tpu as pltpu
from jax.sharding import PartitionSpec as P

HEAD_DIM = 64
WIN = 128
LANES = 128
THETA = 150000.0
EPSILON = 1e-05
MESH = pl.DeviceIdType.MESH
F32 = jnp.float32
BF16 = jnp.bfloat16
QUERY_CUTS = 5
OUT_STEP = 256
HOP_CUTS = 3
SECOND_ORDER = (
    "e0", "f", "q0", "r", "f", "r", "f", "f", "a0", "w0", "o00", "r",
    "e1", "r", "q1", "w1", "o01", "r", "f", "w2", "o02", "a1", "o10", "o11", "o12",
)
AHEAD = 3


def query_pieces(length):
    size = length // QUERY_CUTS
    small = size // 3
    edges = [(0, small), (small, size - small)]
    return edges + [(k * size, size) for k in range(1, QUERY_CUTS)]


def out_pieces(width):
    direct = width % LANES + LANES
    coarse = (width - direct) // OUT_STEP * OUT_STEP
    edges = [(c, OUT_STEP) for c in range(0, coarse - OUT_STEP, OUT_STEP)]
    edges += [(c, LANES) for c in range(coarse - OUT_STEP, width - direct, LANES)]
    return edges + [(width - direct, direct)]


def kernel(
    shape,
    small_ref, small_row,
    tokens_hbm, pair_hbm, query_hbm, out_hbm,
    hidden_ref, cache_ref,
    tokens_ref, pair_ref, out_t, cos_tab, sin_tab,
    query_w, out_w, arrive, window, hbuf, normed_ref, qbuf, cbuf, sink_rows,
    gathered, tq, kd_buf, vd_buf, ctx, outgoing, incoming, final, acc,
    local_sem, x_send, x_recv, y_send, y_recv, d_send, d_recv, own_send, own_recv,
    w_send, w_recv, z_send, z_recv,
    ax_send, ax_recv, ad_send, ad_recv, rd_send, rd_recv, rx_send, rx_recv,
):
    groups, sections, seq = shape
    chips = seq // 2
    g = lax.axis_index("groups")
    sec = lax.axis_index("section")
    q = lax.axis_index("seq")
    chip, core = q // 2, q % 2
    partner = chip * 2 + (1 - core)
    micro, rows, width = hidden_ref.shape
    shard = query_w.shape[2]
    heads_width = seq * shard
    kv_width = pair_ref.shape[1] // 2
    kv_heads = kv_width // HEAD_DIM
    group = heads_width // kv_width
    keep = min(WIN, rows)
    depth = WIN // keep
    span = WIN + rows
    total = seq * rows
    half = HEAD_DIM // 2
    own_heads = shard // HEAD_DIM

    query_rows = width // groups
    query_edges = query_pieces(query_rows)
    out_rows = shard // groups
    out_edges = out_pieces(width)
    last_edge = out_edges[-1]
    cuts = (len(query_edges), len(out_edges) - 1, 1)

    def query_load(j, k):
        first = pl.multiple_of(((g + j) % groups) * query_rows + query_edges[k][0], 16)
        size = query_edges[k][1]
        return pltpu.make_async_copy(
            query_hbm.at[pl.ds(first, size)], query_w.at[q, pl.ds(first, size)],
            local_sem.at[j * cuts[0] + k],
        )

    base = groups * cuts[0]
    out_load = pltpu.make_async_copy(out_hbm, out_t, local_sem.at[base])
    pair_load = pltpu.make_async_copy(pair_hbm, pair_ref, local_sem.at[base + 1])
    tokens_load = pltpu.make_async_copy(tokens_hbm, tokens_ref, local_sem.at[base + 2])

    @pl.when(sec == 0)
    def _():
        tokens_load.start()

    for j in range(groups):
        for k in range(cuts[0]):
            query_load(j, k).start()
    out_load.start()
    pair_load.start()

    barrier = pltpu.get_barrier_semaphore()
    greeted = 0
    for d in range(1, seq):
        pl.semaphore_signal(barrier, 1, device_id={"seq": (q + d) % seq}, device_id_type=MESH)
        greeted += 1
    for e in range(1, groups):
        pl.semaphore_signal(barrier, 1, device_id={"groups": (g + e) % groups}, device_id_type=MESH)
        greeted += 1
    for s in sorted({1 % sections, (sections - 1) % sections} - {0}):
        pl.semaphore_signal(barrier, 1, device_id={"section": (sec + s) % sections}, device_id_type=MESH)
        greeted += 1
    pl.semaphore_wait(barrier, greeted)

    def remote(src, dst, send, recv, target):
        return pltpu.make_async_remote_copy(
            src_ref=src, dst_ref=dst, send_sem=send, recv_sem=recv,
            device_id=target, device_id_type=MESH,
        )

    def source(d, which):
        return ((chip - d + chips) % chips) * 2 + which

    def ahead(d, which):
        return ((chip + d) % chips) * 2 + which

    def own_rows(owner):
        return pl.ds(pl.multiple_of(owner * shard, shard), shard)

    def piece(kind, owner, part, k):
        if kind == 0:
            first = part * query_rows + query_edges[k][0]
            return query_w.at[owner, pl.ds(pl.multiple_of(first, 16), query_edges[k][1])]
        if kind == 2:
            return out_w.at[own_rows(owner), pl.ds(*last_edge)]
        first = pl.multiple_of(owner * shard + part * out_rows, out_rows)
        return out_w.at[pl.ds(first, out_rows), pl.ds(*out_edges[k])]

    def whole(kind, owner):
        if kind == 0:
            return query_w.at[owner]
        return out_w.at[own_rows(owner)]

    slots = (0, cuts[0], cuts[0] + cuts[1])

    def x_copy(kind, d, k, owner):
        ref = piece(kind, owner, g, k)
        return remote(ref, ref, x_send.at[kind, d - 1], x_recv.at[d - 1, slots[kind] + k], {"seq": ahead(d, core)})

    def y_copy(kind, d, k, e, owner, part):
        ref = piece(kind, owner, part, k)
        return remote(
            ref, ref, y_send.at[kind, d - 1, e - 1], y_recv.at[d - 1, slots[kind] + k, e - 1], {"groups": (g + e) % groups}
        )

    def d_copy(kind, d, k, e, owner):
        ref = piece(kind, owner, (g - e + groups) % groups, k)
        return remote(ref, ref, d_send.at[kind], d_recv.at[0 if kind == 0 else slots[kind] - slots[1] + 1 + k], {"seq": partner})

    def part_of(kind, owner, part):
        if kind == 0:
            return query_w.at[owner, pl.ds(pl.multiple_of(part * query_rows, 16), query_rows)]
        if kind == 2:
            return piece(2, owner, part, 0)
        first = pl.multiple_of(owner * shard + part * out_rows, out_rows)
        return out_w.at[pl.ds(first, out_rows), pl.ds(0, last_edge[0])]

    def sent(ref, sem):
        remote(ref, ref, sem, sem, {"seq": partner}).wait_send()

    def landed(ref, sem):
        remote(ref, ref, sem, sem, {"seq": partner}).wait_recv()

    def own_copy(kind, owner):
        ref = whole(kind, owner)
        return remote(ref, ref, own_send.at[kind], own_recv.at[kind], {"seq": partner})

    step = -(-width // (HOP_CUTS * LANES)) * LANES
    edges = [(c * step, min(step, width - c * step)) for c in range(HOP_CUTS)]

    def z_copy(t, c):
        columns = pl.ds(*edges[c])
        return remote(
            hidden_ref.at[t, :, columns], arrive.at[t, :, columns],
            z_send.at[0], z_recv.at[t], {"section": (sec + 1) % sections},
        )

    def w_copy(t, off):
        return remote(
            cache_ref.at[t, pl.ds(rows - keep, keep)], window.at[t, off - 1],
            w_send.at[off - 1], w_recv.at[t, off - 1], {"seq": (q + off) % seq},
        )

    def ax_copy(t, d, owner):
        ref = gathered.at[t, owner]
        return remote(ref, ref, ax_send.at[d - 1], ax_recv.at[t, d - 1], {"seq": ahead(d, core)})

    def ad_copy(t, d, owner):
        ref = gathered.at[t, owner]
        return remote(ref, ref, ad_send.at[0], ad_recv.at[t], {"seq": partner})

    def rd_copy(t, d):
        return remote(
            outgoing.at[t, d], incoming.at[t, d], rd_send.at[0], rd_recv.at[t, d], {"seq": partner}
        )

    def rx_copy(t, d, c):
        columns = pl.ds(*edges[c])
        return remote(
            incoming.at[t, d, :, columns], final.at[t, d, :, columns],
            rx_send.at[d - 1], rx_recv.at[t, d - 1, c], {"seq": ahead(d, core)},
        )

    after = width + heads_width // HEAD_DIM

    def order_of(t):
        return small_ref[0, after + t]

    def length_of(t):
        length = small_ref[0, after + micro]
        for b in range(1, micro):
            length = jnp.where(order_of(t) == b, small_ref[0, after + micro + b], length)
        return length

    def tables(r):
        lane = lax.broadcasted_iota(jnp.int32, (rows, LANES), 1)
        place = lax.broadcasted_iota(jnp.int32, (rows, LANES), 0) + r * rows
        freq = jnp.exp((lane % half).astype(F32) * (-2.0 * math.log(THETA) / HEAD_DIM))
        angles = place.astype(F32) * freq
        at = pl.ds(pl.multiple_of(r * rows, rows), rows)
        cos_tab[at] = jnp.cos(angles)
        sine = jnp.sin(angles)
        sin_tab[at] = jnp.where((lane % HEAD_DIM) < half, -sine, sine)

    def rotate(tile, cosine, sine):
        lane = lax.broadcasted_iota(jnp.int32, tile.shape, 1)
        first_half = (lane % HEAD_DIM) < half
        swapped = jnp.where(
            first_half, pltpu.roll(tile, LANES - half, 1), pltpu.roll(tile, half, 1)
        )
        return tile * cosine + swapped * sine

    def norm(h):
        widened = h.astype(F32)
        scale = lax.rsqrt(jnp.mean(widened * widened, -1, keepdims=True) + EPSILON)
        return (widened * scale * small_row[:, :width]).astype(BF16)

    def transpose_out():
        out_load.wait()
        for first in range(0, width, LANES):
            size = min(LANES, width - first)
            out_w[own_rows(q), first:first + size] = out_t[first:first + size, :].T

    def bias_of(r, length, lanes):
        key = lax.broadcasted_iota(jnp.int32, (span, lanes), 0) - WIN
        row = lax.broadcasted_iota(jnp.int32, (span, lanes), 1) % rows
        column = key + r * rows
        allowed = (key <= row) & (row - key < WIN) & (column >= 0)
        allowed = allowed & ((column.astype(F32) < length) | (key == row))
        return jnp.where(allowed, F32(0.0), F32(-1e30))

    def sink_row(first, tiles):
        return jnp.concatenate(
            [jnp.full((1, rows), small_ref[0, width + first + 2 * p], F32) for p in range(tiles)], 1
        )

    low = lax.broadcasted_iota(jnp.int32, (span, LANES), 1) < HEAD_DIM
    ones = jnp.ones((16, span), BF16)

    def attention(jobs):
        scores = []
        for pairs, twice, _, _, _ in jobs:
            zero = jnp.zeros_like(twice)
            sides = jnp.concatenate([jnp.where(low, twice, zero), jnp.where(low, zero, twice)], 0)
            scores.append(lax.dot_general(
                sides, jnp.concatenate(pairs, 0), (((1,), (1,)), ((), ())),
                preferred_element_type=F32,
            ))
        results = []
        for (_, _, values_t, bias, sinks), score in zip(jobs, scores):
            extended = jnp.concatenate([values_t, ones], 0)
            parts = []
            for b in range(2):
                masked = score[b * span:(b + 1) * span] + bias
                top = jnp.maximum(jnp.max(masked, 0, keepdims=True), sinks[b])
                expo = jnp.exp(masked - top).astype(BF16)
                summed = jnp.dot(extended, expo, preferred_element_type=F32)
                whole_sum = summed[HEAD_DIM:HEAD_DIM + 1] + jnp.exp(sinks[b] - top)
                parts.append(summed[:HEAD_DIM] * (1.0 / whole_sum))
            results.append(jnp.concatenate(parts, 0).T.astype(BF16))
        return results

    def cache_of(t, normed, cosine, sine, send):
        keys = jnp.dot(normed, pair_ref[:, :kv_width], preferred_element_type=F32)
        for p in range(kv_width // LANES):
            tile = slice(p * LANES, (p + 1) * LANES)
            cache_ref[t, :, tile] = rotate(keys[:, tile], cosine, sine).astype(BF16)
        values = jnp.dot(normed, pair_ref[:, kv_width:], preferred_element_type=F32)
        cache_ref[t, :, kv_width:] = values.astype(BF16)
        if send:
            for off in range(1, depth + 1):

                @pl.when(q + off < seq)
                def _():
                    w_copy(t, off).start()

    mine = pl.ds(pl.multiple_of(q * rows, rows), rows)

    def first_section():
        tiles = shard // LANES
        tokens_load.wait()
        for t in range(micro):
            block = tokens_ref[0]
            for b in range(1, micro):
                block = jnp.where(order_of(t) == b, tokens_ref[b], block)
            hbuf[t] = block
            gathered[t, q] = norm(hbuf[t])
            if t < micro - 1 or micro < 3:
                for d in range(1, chips):
                    ax_copy(t, d, q).start()
            ad_copy(t, 0, q).start()
        for r in range(seq):
            tables(r)
        kd_buf[:WIN] = jnp.zeros((WIN, LANES), BF16)
        vd_buf[:WIN] = jnp.zeros((WIN, LANES), BF16)
        transpose_out()
        pair_load.wait()
        for j in range(groups):
            for k in range(cuts[0]):
                query_load(j, k).wait()
        for t in range(micro):
            cache_of(t, gathered[t, q], cos_tab[mine], sin_tab[mine], False)

        kv_head = (q * own_heads) // group
        pair_at = pl.ds(pl.multiple_of((kv_head // 2) * LANES, LANES), LANES)
        value_at = pl.ds(pl.multiple_of(kv_width + (kv_head // 2) * LANES, LANES), LANES)
        sinks = [sink_row(q * own_heads + b, tiles) for b in range(2)]

        def double(tile):
            lane = lax.broadcasted_iota(jnp.int32, tile.shape, 1)
            kept = jnp.where(lane // HEAD_DIM == kv_head % 2, tile, 0.0)
            return (kept + pltpu.roll(kept, HEAD_DIM, 1)).astype(BF16)

        def finish(t):
            rd_copy(t, 0).wait_recv()
            for c, (first, size) in enumerate(edges):
                columns = slice(first, first + size)
                joined = acc[t, :, columns] + incoming[t, 0, :, columns].astype(F32)
                for d in range(1, chips):
                    rx_copy(t, d, c).wait_recv()
                    joined = joined + final[t, d, :, columns].astype(F32)
                hidden_ref[t, :, columns] = joined.astype(BF16)
                if sections > 1:
                    z_copy(t, c).start()

        def compute(t):
            for d in range(1, chips):
                ax_copy(t, d, source(d, core)).wait_recv()
                ad_copy(t, d, source(d, core)).start()
            landed(outgoing.at[t], ad_recv.at[t])
            length = length_of(t)
            normed = gathered[t].reshape(total, width)
            cosine, sine = cos_tab[...], sin_tab[...]
            keys = jnp.dot(normed, pair_ref[:, pair_at], preferred_element_type=F32)
            kd_buf[WIN:] = double(rotate(keys, cosine, sine))
            vd_buf[WIN:] = double(jnp.dot(normed, pair_ref[:, value_at], preferred_element_type=F32))
            queries = jnp.dot(normed, query_w[q], preferred_element_type=F32)
            for p in range(tiles):
                tile = slice(p * LANES, (p + 1) * LANES)
                tq[:, tile] = (rotate(queries[:, tile], cosine, sine) * 0.125).astype(BF16)
            jobs = []
            for r in range(seq):
                at = slice(r * rows, r * rows + span)
                jobs.append((
                    [tq[r * rows:(r + 1) * rows, p * LANES:(p + 1) * LANES] for p in range(tiles)],
                    kd_buf[at], vd_buf[at].T[:HEAD_DIM], bias_of(r, length, tiles * rows), sinks,
                ))
            for r, some in enumerate(attention(jobs)):
                for p in range(tiles):
                    ctx[r, :, p * LANES:(p + 1) * LANES] = some[p * rows:(p + 1) * rows]

            if micro >= 3:

                @pl.when(t == micro - 1)
                def _():
                    finish(1)

            weights = out_w[own_rows(q), :]
            there = jnp.dot(
                jnp.concatenate([ctx[ahead(d, 1 - core)] for d in range(chips)], 0), weights,
                preferred_element_type=F32,
            )
            for d in list(range(1, chips)) + [0]:
                outgoing[t, d] = there[d * rows:(d + 1) * rows].astype(BF16)
                rd_copy(t, d).start()
            here = jnp.dot(
                jnp.concatenate([ctx[ahead(d, core)] for d in range(chips)], 0), weights,
                preferred_element_type=F32,
            )
            acc[t] = hbuf[t].astype(F32) + here[:rows]
            for d in range(1, chips):
                rd_copy(t, d).wait_recv()
                joined = here[d * rows:(d + 1) * rows] + incoming[t, d].astype(F32)
                incoming[t, d] = joined.astype(BF16)
                for c in range(HOP_CUTS):
                    rx_copy(t, d, c).start()

        @pl.loop(0, micro)
        def _(t):
            if micro >= 3:

                @pl.when(t == 2)
                def _():
                    finish(0)

            compute(t)
            if micro >= 3:

                @pl.when(t == 0)
                def _():
                    for d in range(1, chips):
                        ax_copy(micro - 1, d, q).start()

        @pl.loop(2 if micro >= 3 else 0, micro)
        def _(t):
            finish(t)

        for d in range(1, chips):
            sent(gathered.at[:, q], ax_send.at[d - 1])
            sent(incoming.at[:, d], rx_send.at[d - 1])
        sent(outgoing, ad_send.at[0])
        sent(outgoing, rd_send.at[0])

    def later_section():
        tiles = group // 2
        for k in range(cuts[0]):
            query_load(0, k).wait()
            for d in range(1, chips):
                x_copy(0, d, k, q).start()
        transpose_out()
        rounds = [(kind, k) for kind in range(3) for k in range(cuts[kind])]
        outs = rounds[cuts[0]:]

        def send_out(one):
            for d in range(1, chips):
                x_copy(one[0], d, one[1], q).start()

        for one in outs[:AHEAD]:
            send_out(one)

        @pl.when(sec > 1)
        def _():
            for one in outs[AHEAD:]:
                send_out(one)

        for j in range(1, groups):
            for k in range(cuts[0]):
                query_load(j, k).wait()
        for kind in range(2):
            own_copy(kind, q).start()
        tables(q)
        for off in range(1, depth + 1):

            @pl.when(q < off)
            def _():
                window[:, off - 1] = jnp.zeros((micro, keep, 2 * kv_width), BF16)

        for h in range(kv_heads):
            for b in range(2):
                sink_rows[2 * h + b:2 * h + b + 1, :] = sink_row(h * group + b, tiles)
        pair_load.wait()

        def forward(kind, k):
            for d in range(1, chips):
                x_copy(kind, d, k, source(d, core)).wait_recv()
                if kind < 2:
                    for e in range(1, groups):
                        y_copy(kind, d, k, e, source(d, core), g).start()
                d_copy(kind, d, k, 0, source(d, core)).start()

        def relay(kind, k):
            if kind < 2:
                for d in range(1, chips):
                    for e in range(1, groups):
                        y_copy(kind, d, k, e, source(d, core), (g - e + groups) % groups).wait_recv()
                        d_copy(kind, d, k, e, source(d, core)).start()

        def several(first, size):
            return out_w.at[pl.ds(0, (chips - 1) * shard), pl.ds(first, size)]

        def ready_queries():
            own_copy(0, partner).wait_recv()
            if chips > 1:
                landed(query_w.at[pl.ds(0, chips - 1)], d_recv.at[0])

        def ready(k):
            if k == 0:
                own_copy(1, partner).wait_recv()
            if chips > 1:
                landed(several(*out_edges[k]), d_recv.at[1 + k])

        def gather_sent():
            for kind in range(3):
                for d in range(1, chips):
                    sent(part_of(kind, q, g), x_send.at[kind, d - 1])
                    for e in range(1, groups if kind < 2 else 1):
                        sent(part_of(kind, source(d, core), g), y_send.at[kind, d - 1, e - 1])
            if chips > 1:
                sent(query_w.at[pl.ds(0, chips - 1)], d_send.at[0])
                sent(several(0, last_edge[0]), d_send.at[1])
                sent(several(*last_edge), d_send.at[2])
            for kind in range(2):
                own_copy(kind, q).wait_send()

        def enter(t):
            landed(arrive.at[t], z_recv.at[t])
            normed_ref[t] = norm(arrive[t])
            cache_of(t, normed_ref[t], cos_tab[mine], sin_tab[mine], True)

        def ask(t):
            normed = normed_ref[t]
            cosine, sine = cos_tab[mine], sin_tab[mine]
            for s in range(seq):
                queries = jnp.dot(normed, query_w[s], preferred_element_type=F32)
                for p in range(shard // LANES):
                    rotated = rotate(queries[:, p * LANES:(p + 1) * LANES], cosine, sine) * 0.125
                    qbuf[:, s * shard + p * LANES:s * shard + (p + 1) * LANES] = rotated.astype(BF16)

        def attend(t):
            length = length_of(t)
            for off in range(1, depth + 1):

                @pl.when(q >= off)
                def _():
                    landed(window.at[t, off - 1], w_recv.at[t, off - 1])

            bias = bias_of(q, length, tiles * rows)

            def span_of(first, size):
                at = slice(first, first + size)
                parts = [window[t, off - 1, :, at] for off in range(depth, 0, -1)]
                return jnp.concatenate(parts + [cache_ref[t, :, at]], 0)

            jobs = []
            for pair in range(kv_heads // 2):
                values_t = span_of(kv_width + pair * LANES, LANES).T
                for e in range(2):
                    h = pair * 2 + e
                    head = span_of(h * HEAD_DIM, HEAD_DIM)
                    jobs.append((
                        [qbuf[:, a:a + LANES] for a in range(h * tiles * LANES, (h + 1) * tiles * LANES, LANES)],
                        jnp.concatenate([head, head], 1),
                        values_t[e * HEAD_DIM:(e + 1) * HEAD_DIM], bias,
                        [sink_rows[2 * h + b:2 * h + b + 1, :] for b in range(2)],
                    ))
            for h, some in enumerate(attention(jobs)):
                for p in range(tiles):
                    at = (h * tiles + p) * LANES
                    cbuf[t, :, at:at + LANES] = some[p * rows:(p + 1) * rows]

        def leave(t, c, send=True):
            first, size = edges[c]
            columns = slice(first, first + size)
            output = jnp.dot(cbuf[t], out_w[:, columns], preferred_element_type=F32)
            hidden_ref[t, :, columns] = (arrive[t, :, columns].astype(F32) + output).astype(BF16)
            if send:
                z_copy(t, c).start()

        needed = [[] for c in range(HOP_CUTS)]
        for k, (first, size) in enumerate(out_edges):
            needed[first // step].append(k)

        @pl.when(sec == 1)
        def _():
            waiting, relayed = list(rounds), []

            def forward_next():
                if waiting:
                    one = waiting.pop(0)
                    forward(*one)
                    at = rounds.index(one) + AHEAD
                    if one[0] and at < len(rounds):
                        send_out(rounds[at])
                    relayed.append(one)

            def relay_next():
                if relayed:
                    relay(*relayed.pop(0))

            while len(waiting) > len(outs) - 2:
                forward_next()
                if len(relayed) > 1:
                    relay_next()
            while relayed and relayed[0][0] == 0:
                relay_next()
            ready_queries()
            for what in SECOND_ORDER:
                if what[0] == "f":
                    forward_next()
                elif what[0] == "r":
                    relay_next()
                elif what[0] == "w":
                    for k in needed[int(what[1])]:
                        ready(k)
                elif what[0] == "o":
                    leave(int(what[1]), int(what[2]), False)

                    @pl.when(sec + 1 < sections)
                    def _():
                        z_copy(int(what[1]), int(what[2])).start()

                else:
                    (enter, ask, attend)["eqa".index(what[0])](int(what[1]))

        @pl.when(sec > 1)
        def _():
            previous = None
            for one in rounds:
                forward(*one)
                if previous is not None:
                    relay(*previous)
                previous = one
            relay(*previous)
            ready_queries()
            for k in range(len(out_edges)):
                ready(k)
            gather_sent()

        def slot(send, t, carry):
            enter(t)
            ask(t)
            attend(t)
            for c in range(HOP_CUTS):
                leave(t, c, send)
            return carry

        start = jnp.where(sec == 1, 2, 0)

        @pl.when(sec + 1 < sections)
        def _():
            lax.fori_loop(start, micro, functools.partial(slot, True), 0)

        @pl.when(sec + 1 == sections)
        def _():
            lax.fori_loop(start, micro, functools.partial(slot, False), 0)

        @pl.when(sec == 1)
        def _():
            gather_sent()

        for off in range(1, depth + 1):

            @pl.when(q + off < seq)
            def _():
                sent(window.at[:, off - 1], w_send.at[off - 1])

    @pl.when(sec == 0)
    def _():
        first_section()

    @pl.when(sec > 0)
    def _():
        later_section()

    @pl.when(sec + 1 < sections)
    def _():
        sent(arrive, z_send.at[0])


def per_device(
    shape,
    tokens, block_order, prompt_lengths, norm_gain, w_query, w_key_value, w_out, sink_logits
):
    groups, sections, seq = shape
    micro, rows, width = tokens.shape
    shard = w_query.shape[2]
    pair_width = w_key_value.shape[2]
    kv_heads = pair_width // 2 // HEAD_DIM
    lanes = seq * shard // (pair_width // 2) // 2 * rows
    chips = seq // 2
    keep = min(WIN, rows)
    depth = WIN // keep
    others, peers = max(1, chips - 1), max(1, groups - 1)
    queries = len(query_pieces(width // groups))
    rounds = queries + len(out_pieces(width))
    limit = 55488512 if seq * rows <= 512 else 57 * 1024 * 1024
    parts = [norm_gain, sink_logits, block_order[None].astype(F32), prompt_lengths[None].astype(F32)]
    small_width = sum(part.shape[1] for part in parts)
    small, first = 0.0, 0
    for part in parts:
        behind = small_width - first - part.shape[1]
        small = small + jnp.pad(part, ((0, 0), (first, behind)))
        first += part.shape[1]
    dma = pltpu.SemaphoreType.DMA
    vmem = pl.BlockSpec(memory_space=pltpu.VMEM)
    smem = pl.BlockSpec(memory_space=pltpu.SMEM)
    hbm = pl.BlockSpec(memory_space=pltpu.HBM)
    hidden, cache = pl.pallas_call(
        functools.partial(kernel, shape),
        out_shape=(
            jax.ShapeDtypeStruct((micro, rows, width), BF16),
            jax.ShapeDtypeStruct((micro, rows, pair_width), BF16),
        ),
        in_specs=[smem, vmem] + [hbm] * 4,
        out_specs=(vmem, vmem),
        scratch_shapes=[
            pltpu.VMEM((micro, rows, width), BF16),
            pltpu.VMEM((width, pair_width), BF16),
            pltpu.VMEM((width, shard), BF16),
            pltpu.VMEM((seq * rows, LANES), F32),
            pltpu.VMEM((seq * rows, LANES), F32),
            pltpu.VMEM((seq, width, shard), BF16),
            pltpu.VMEM((seq * shard, width), BF16),
            pltpu.VMEM((micro, rows, width), BF16),
            pltpu.VMEM((micro, depth, keep, pair_width), BF16),
            pltpu.VMEM((micro, rows, width), BF16),
            pltpu.VMEM((micro, rows, width), BF16),
            pltpu.VMEM((rows, seq * shard), BF16),
            pltpu.VMEM((micro, rows, seq * shard), BF16),
            pltpu.VMEM((2 * kv_heads, lanes), F32),
            pltpu.VMEM((micro, seq, rows, width), BF16),
            pltpu.VMEM((seq * rows, shard), BF16),
            pltpu.VMEM((WIN + seq * rows, LANES), BF16),
            pltpu.VMEM((WIN + seq * rows, LANES), BF16),
            pltpu.VMEM((seq, rows, shard), BF16),
            pltpu.VMEM((micro, chips, rows, width), BF16),
            pltpu.VMEM((micro, chips, rows, width), BF16),
            pltpu.VMEM((micro, chips, rows, width), BF16),
            pltpu.VMEM((micro, rows, width), F32),
            dma((groups * queries + 3,)),
            dma((3, others)),
            dma((others, rounds)),
            dma((3, others, peers)),
            dma((others, rounds, peers)),
            dma((3,)),
            dma((rounds,)),
            dma((2,)),
            dma((2,)),
            dma((depth,)),
            dma((micro, depth)),
            dma((1,)),
            dma((micro,)),
            dma((others,)),
            dma((micro, others)),
            dma((1,)),
            dma((micro,)),
            dma((1,)),
            dma((micro, chips)),
            dma((others,)),
            dma((micro, others, HOP_CUTS)),
        ],
        compiler_params=pltpu.CompilerParams(
            collective_id=0, has_side_effects=True, vmem_limit_bytes=limit
        ),
    )(
        small, small,
        tokens, w_key_value[0], w_query[0], w_out[0].T,
    )
    return hidden[None], cache[None]


def solution(mesh):
    in_specs = (
        P("groups", "seq", None),
        P("groups"),
        P("groups"),
        P("section", None),
        P("section", None, "seq"),
        P("section", None, None),
        P("section", "seq", None),
        P("section", None),
    )
    out_specs = (P("section", "groups", "seq", None), P("section", "groups", "seq", None))
    shape = tuple(mesh.shape[name] for name in ("groups", "section", "seq"))
    return jax.shard_map(
        functools.partial(per_device, shape),
        mesh=mesh, in_specs=in_specs, out_specs=out_specs, check_vma=False,
    )
```

```python
import functools
import math

import jax
import jax.numpy as jnp
from jax import lax
from jax.experimental import pallas as pl
from jax.experimental.pallas import tpu as pltpu
from jax.sharding import PartitionSpec as P

HEAD_DIM = 64
WIN = 128
LANES = 128
THETA = 150000.0
EPSILON = 1e-05
MESH = pl.DeviceIdType.MESH
F32 = jnp.float32
BF16 = jnp.bfloat16
QUERY_CUTS = 5
OUT_STEP = 256
HOP_CUTS = 3
SECOND_ORDER = (
    "e0", "f", "q0", "r", "f", "r", "f", "f", "a0", "w0", "o00", "r",
    "e1", "r", "q1", "w1", "o01", "r", "f", "w2", "o02", "a1", "o10", "o11", "o12",
)
AHEAD = 3


def query_pieces(length):
    size = length // QUERY_CUTS
    small = size // 3
    edges = [(0, small), (small, size - small)]
    return edges + [(k * size, size) for k in range(1, QUERY_CUTS)]


def out_pieces(width):
    direct = width % LANES + LANES
    coarse = (width - direct) // OUT_STEP * OUT_STEP
    edges = [(c, OUT_STEP) for c in range(0, coarse - OUT_STEP, OUT_STEP)]
    edges += [(c, LANES) for c in range(coarse - OUT_STEP, width - direct, LANES)]
    return edges + [(width - direct, direct)]


def kernel(
    shape,
    small_ref, small_row,
    tokens_hbm, pair_hbm, query_hbm, out_hbm,
    hidden_ref, cache_ref,
    tokens_ref, pair_ref, out_t, cos_tab, sin_tab,
    query_w, out_w, arrive, window, hbuf, normed_ref, qbuf, cbuf, sink_rows,
    gathered, tq, kd_buf, vd_buf, ctx, outgoing, incoming, final, acc,
    local_sem, x_send, x_recv, y_send, y_recv, d_send, d_recv, own_send, own_recv,
    w_send, w_recv, z_send, z_recv,
    ax_send, ax_recv, ad_send, ad_recv, rd_send, rd_recv, rx_send, rx_recv,
):
    groups, sections, seq = shape
    chips = seq // 2
    g = lax.axis_index("groups")
    sec = lax.axis_index("section")
    q = lax.axis_index("seq")
    chip, core = q // 2, q % 2
    partner = chip * 2 + (1 - core)
    micro, rows, width = hidden_ref.shape
    shard = query_w.shape[2]
    heads_width = seq * shard
    kv_width = pair_ref.shape[1] // 2
    kv_heads = kv_width // HEAD_DIM
    group = heads_width // kv_width
    keep = min(WIN, rows)
    depth = WIN // keep
    span = WIN + rows
    total = seq * rows
    half = HEAD_DIM // 2
    own_heads = shard // HEAD_DIM

    query_rows = width // groups
    query_edges = query_pieces(query_rows)
    out_rows = shard // groups
    out_edges = out_pieces(width)
    last_edge = out_edges[-1]
    cuts = (len(query_edges), len(out_edges) - 1, 1)

    def query_load(j, k):
        first = pl.multiple_of(((g + j) % groups) * query_rows + query_edges[k][0], 16)
        size = query_edges[k][1]
        return pltpu.make_async_copy(
            query_hbm.at[pl.ds(first, size)], query_w.at[q, pl.ds(first, size)],
            local_sem.at[j * cuts[0] + k],
        )

    base = groups * cuts[0]
    out_load = pltpu.make_async_copy(out_hbm, out_t, local_sem.at[base])
    pair_load = pltpu.make_async_copy(pair_hbm, pair_ref, local_sem.at[base + 1])
    tokens_load = pltpu.make_async_copy(tokens_hbm, tokens_ref, local_sem.at[base + 2])

    @pl.when(sec == 0)
    def _():
        tokens_load.start()

    for j in range(groups):
        for k in range(cuts[0]):
            query_load(j, k).start()
    out_load.start()
    pair_load.start()

    barrier = pltpu.get_barrier_semaphore()
    greeted = 0
    for d in range(1, seq):
        pl.semaphore_signal(barrier, 1, device_id={"seq": (q + d) % seq}, device_id_type=MESH)
        greeted += 1
    for e in range(1, groups):
        pl.semaphore_signal(barrier, 1, device_id={"groups": (g + e) % groups}, device_id_type=MESH)
        greeted += 1
    for s in sorted({1 % sections, (sections - 1) % sections} - {0}):
        pl.semaphore_signal(barrier, 1, device_id={"section": (sec + s) % sections}, device_id_type=MESH)
        greeted += 1
    pl.semaphore_wait(barrier, greeted)

    def remote(src, dst, send, recv, target):
        return pltpu.make_async_remote_copy(
            src_ref=src, dst_ref=dst, send_sem=send, recv_sem=recv,
            device_id=target, device_id_type=MESH,
        )

    def source(d, which):
        return ((chip - d + chips) % chips) * 2 + which

    def ahead(d, which):
        return ((chip + d) % chips) * 2 + which

    def own_rows(owner):
        return pl.ds(pl.multiple_of(owner * shard, shard), shard)

    def piece(kind, owner, part, k):
        if kind == 0:
            first = part * query_rows + query_edges[k][0]
            return query_w.at[owner, pl.ds(pl.multiple_of(first, 16), query_edges[k][1])]
        if kind == 2:
            return out_w.at[own_rows(owner), pl.ds(*last_edge)]
        first = pl.multiple_of(owner * shard + part * out_rows, out_rows)
        return out_w.at[pl.ds(first, out_rows), pl.ds(*out_edges[k])]

    def whole(kind, owner):
        if kind == 0:
            return query_w.at[owner]
        return out_w.at[own_rows(owner)]

    slots = (0, cuts[0], cuts[0] + cuts[1])

    def x_copy(kind, d, k, owner):
        ref = piece(kind, owner, g, k)
        return remote(ref, ref, x_send.at[kind, d - 1], x_recv.at[d - 1, slots[kind] + k], {"seq": ahead(d, core)})

    def y_copy(kind, d, k, e, owner, part):
        ref = piece(kind, owner, part, k)
        return remote(
            ref, ref, y_send.at[kind, d - 1, e - 1], y_recv.at[d - 1, slots[kind] + k, e - 1], {"groups": (g + e) % groups}
        )

    def d_copy(kind, d, k, e, owner):
        ref = piece(kind, owner, (g - e + groups) % groups, k)
        return remote(ref, ref, d_send.at[kind], d_recv.at[0 if kind == 0 else slots[kind] - slots[1] + 1 + k], {"seq": partner})

    def part_of(kind, owner, part):
        if kind == 0:
            return query_w.at[owner, pl.ds(pl.multiple_of(part * query_rows, 16), query_rows)]
        if kind == 2:
            return piece(2, owner, part, 0)
        first = pl.multiple_of(owner * shard + part * out_rows, out_rows)
        return out_w.at[pl.ds(first, out_rows), pl.ds(0, last_edge[0])]

    def sent(ref, sem):
        remote(ref, ref, sem, sem, {"seq": partner}).wait_send()

    def landed(ref, sem):
        remote(ref, ref, sem, sem, {"seq": partner}).wait_recv()

    def own_copy(kind, owner):
        ref = whole(kind, owner)
        return remote(ref, ref, own_send.at[kind], own_recv.at[kind], {"seq": partner})

    step = -(-width // (HOP_CUTS * LANES)) * LANES
    edges = [(c * step, min(step, width - c * step)) for c in range(HOP_CUTS)]

    def z_copy(t, c):
        columns = pl.ds(*edges[c])
        return remote(
            hidden_ref.at[t, :, columns], arrive.at[t, :, columns],
            z_send.at[0], z_recv.at[t], {"section": (sec + 1) % sections},
        )

    def w_copy(t, off):
        return remote(
            cache_ref.at[t, pl.ds(rows - keep, keep)], window.at[t, off - 1],
            w_send.at[off - 1], w_recv.at[t, off - 1], {"seq": (q + off) % seq},
        )

    def ax_copy(t, d, owner):
        ref = gathered.at[t, owner]
        return remote(ref, ref, ax_send.at[d - 1], ax_recv.at[t, d - 1], {"seq": ahead(d, core)})

    def ad_copy(t, d, owner):
        ref = gathered.at[t, owner]
        return remote(ref, ref, ad_send.at[0], ad_recv.at[t], {"seq": partner})

    def rd_copy(t, d):
        return remote(
            outgoing.at[t, d], incoming.at[t, d], rd_send.at[0], rd_recv.at[t, d], {"seq": partner}
        )

    def rx_copy(t, d, c):
        columns = pl.ds(*edges[c])
        return remote(
            incoming.at[t, d, :, columns], final.at[t, d, :, columns],
            rx_send.at[d - 1], rx_recv.at[t, d - 1, c], {"seq": ahead(d, core)},
        )

    after = width + heads_width // HEAD_DIM

    def order_of(t):
        return small_ref[0, after + t]

    def length_of(t):
        length = small_ref[0, after + micro]
        for b in range(1, micro):
            length = jnp.where(order_of(t) == b, small_ref[0, after + micro + b], length)
        return length

    def tables(r):
        lane = lax.broadcasted_iota(jnp.int32, (rows, LANES), 1)
        place = lax.broadcasted_iota(jnp.int32, (rows, LANES), 0) + r * rows
        freq = jnp.exp((lane % half).astype(F32) * (-2.0 * math.log(THETA) / HEAD_DIM))
        angles = place.astype(F32) * freq
        at = pl.ds(pl.multiple_of(r * rows, rows), rows)
        cos_tab[at] = jnp.cos(angles)
        sine = jnp.sin(angles)
        sin_tab[at] = jnp.where((lane % HEAD_DIM) < half, -sine, sine)

    def rotate(tile, cosine, sine):
        lane = lax.broadcasted_iota(jnp.int32, tile.shape, 1)
        first_half = (lane % HEAD_DIM) < half
        swapped = jnp.where(
            first_half, pltpu.roll(tile, LANES - half, 1), pltpu.roll(tile, half, 1)
        )
        return tile * cosine + swapped * sine

    def norm(h):
        widened = h.astype(F32)
        scale = lax.rsqrt(jnp.mean(widened * widened, -1, keepdims=True) + EPSILON)
        return (widened * scale * small_row[:, :width]).astype(BF16)

    def transpose_out():
        out_load.wait()
        for first in range(0, width, LANES):
            size = min(LANES, width - first)
            out_w[own_rows(q), first:first + size] = out_t[first:first + size, :].T

    def bias_of(r, length, lanes):
        key = lax.broadcasted_iota(jnp.int32, (span, lanes), 0) - WIN
        row = lax.broadcasted_iota(jnp.int32, (span, lanes), 1) % rows
        column = key + r * rows
        allowed = (key <= row) & (row - key < WIN) & (column >= 0)
        allowed = allowed & ((column.astype(F32) < length) | (key == row))
        return jnp.where(allowed, F32(0.0), F32(-1e30))

    def sink_row(first, tiles):
        return jnp.concatenate(
            [jnp.full((1, rows), small_ref[0, width + first + 2 * p], F32) for p in range(tiles)], 1
        )

    low = lax.broadcasted_iota(jnp.int32, (span, LANES), 1) < HEAD_DIM
    ones = jnp.ones((16, span), BF16)

    def attention(jobs):
        scores = []
        for pairs, twice, _, _, _ in jobs:
            zero = jnp.zeros_like(twice)
            sides = jnp.concatenate([jnp.where(low, twice, zero), jnp.where(low, zero, twice)], 0)
            scores.append(lax.dot_general(
                sides, jnp.concatenate(pairs, 0), (((1,), (1,)), ((), ())),
                preferred_element_type=F32,
            ))
        results = []
        for (_, _, values_t, bias, sinks), score in zip(jobs, scores):
            extended = jnp.concatenate([values_t, ones], 0)
            parts = []
            for b in range(2):
                masked = score[b * span:(b + 1) * span] + bias
                top = jnp.maximum(jnp.max(masked, 0, keepdims=True), sinks[b])
                expo = jnp.exp(masked - top).astype(BF16)
                summed = jnp.dot(extended, expo, preferred_element_type=F32)
                whole_sum = summed[HEAD_DIM:HEAD_DIM + 1] + jnp.exp(sinks[b] - top)
                parts.append(summed[:HEAD_DIM] * (1.0 / whole_sum))
            results.append(jnp.concatenate(parts, 0).T.astype(BF16))
        return results

    def cache_of(t, normed, cosine, sine, send):
        keys = jnp.dot(normed, pair_ref[:, :kv_width], preferred_element_type=F32)
        for p in range(kv_width // LANES):
            tile = slice(p * LANES, (p + 1) * LANES)
            cache_ref[t, :, tile] = rotate(keys[:, tile], cosine, sine).astype(BF16)
        values = jnp.dot(normed, pair_ref[:, kv_width:], preferred_element_type=F32)
        cache_ref[t, :, kv_width:] = values.astype(BF16)
        if send:
            for off in range(1, depth + 1):

                @pl.when(q + off < seq)
                def _():
                    w_copy(t, off).start()

    mine = pl.ds(pl.multiple_of(q * rows, rows), rows)

    def first_section():
        tiles = shard // LANES
        tokens_load.wait()
        for t in range(micro):
            block = tokens_ref[0]
            for b in range(1, micro):
                block = jnp.where(order_of(t) == b, tokens_ref[b], block)
            hbuf[t] = block
            gathered[t, q] = norm(hbuf[t])
            if t < micro - 1 or micro < 3:
                for d in range(1, chips):
                    ax_copy(t, d, q).start()
            ad_copy(t, 0, q).start()
        for r in range(seq):
            tables(r)
        kd_buf[:WIN] = jnp.zeros((WIN, LANES), BF16)
        vd_buf[:WIN] = jnp.zeros((WIN, LANES), BF16)
        transpose_out()
        pair_load.wait()
        for j in range(groups):
            for k in range(cuts[0]):
                query_load(j, k).wait()
        for t in range(micro):
            cache_of(t, gathered[t, q], cos_tab[mine], sin_tab[mine], False)

        kv_head = (q * own_heads) // group
        pair_at = pl.ds(pl.multiple_of((kv_head // 2) * LANES, LANES), LANES)
        value_at = pl.ds(pl.multiple_of(kv_width + (kv_head // 2) * LANES, LANES), LANES)
        sinks = [sink_row(q * own_heads + b, tiles) for b in range(2)]

        def double(tile):
            lane = lax.broadcasted_iota(jnp.int32, tile.shape, 1)
            kept = jnp.where(lane // HEAD_DIM == kv_head % 2, tile, 0.0)
            return (kept + pltpu.roll(kept, HEAD_DIM, 1)).astype(BF16)

        def finish(t):
            rd_copy(t, 0).wait_recv()
            for c, (first, size) in enumerate(edges):
                columns = slice(first, first + size)
                joined = acc[t, :, columns] + incoming[t, 0, :, columns].astype(F32)
                for d in range(1, chips):
                    rx_copy(t, d, c).wait_recv()
                    joined = joined + final[t, d, :, columns].astype(F32)
                hidden_ref[t, :, columns] = joined.astype(BF16)
                if sections > 1:
                    z_copy(t, c).start()

        def compute(t):
            for d in range(1, chips):
                ax_copy(t, d, source(d, core)).wait_recv()
                ad_copy(t, d, source(d, core)).start()
            landed(outgoing.at[t], ad_recv.at[t])
            length = length_of(t)
            normed = gathered[t].reshape(total, width)
            cosine, sine = cos_tab[...], sin_tab[...]
            keys = jnp.dot(normed, pair_ref[:, pair_at], preferred_element_type=F32)
            kd_buf[WIN:] = double(rotate(keys, cosine, sine))
            vd_buf[WIN:] = double(jnp.dot(normed, pair_ref[:, value_at], preferred_element_type=F32))
            queries = jnp.dot(normed, query_w[q], preferred_element_type=F32)
            for p in range(tiles):
                tile = slice(p * LANES, (p + 1) * LANES)
                tq[:, tile] = (rotate(queries[:, tile], cosine, sine) * 0.125).astype(BF16)
            jobs = []
            for r in range(seq):
                at = slice(r * rows, r * rows + span)
                jobs.append((
                    [tq[r * rows:(r + 1) * rows, p * LANES:(p + 1) * LANES] for p in range(tiles)],
                    kd_buf[at], vd_buf[at].T[:HEAD_DIM], bias_of(r, length, tiles * rows), sinks,
                ))
            for r, some in enumerate(attention(jobs)):
                for p in range(tiles):
                    ctx[r, :, p * LANES:(p + 1) * LANES] = some[p * rows:(p + 1) * rows]

            if micro >= 3:

                @pl.when(t == micro - 1)
                def _():
                    finish(1)

            weights = out_w[own_rows(q), :]
            there = jnp.dot(
                jnp.concatenate([ctx[ahead(d, 1 - core)] for d in range(chips)], 0), weights,
                preferred_element_type=F32,
            )
            for d in list(range(1, chips)) + [0]:
                outgoing[t, d] = there[d * rows:(d + 1) * rows].astype(BF16)
                rd_copy(t, d).start()
            here = jnp.dot(
                jnp.concatenate([ctx[ahead(d, core)] for d in range(chips)], 0), weights,
                preferred_element_type=F32,
            )
            acc[t] = hbuf[t].astype(F32) + here[:rows]
            for d in range(1, chips):
                rd_copy(t, d).wait_recv()
                joined = here[d * rows:(d + 1) * rows] + incoming[t, d].astype(F32)
                incoming[t, d] = joined.astype(BF16)
                for c in range(HOP_CUTS):
                    rx_copy(t, d, c).start()

        @pl.loop(0, micro)
        def _(t):
            if micro >= 3:

                @pl.when(t == 2)
                def _():
                    finish(0)

            compute(t)
            if micro >= 3:

                @pl.when(t == 0)
                def _():
                    for d in range(1, chips):
                        ax_copy(micro - 1, d, q).start()

        @pl.loop(2 if micro >= 3 else 0, micro)
        def _(t):
            finish(t)

        for d in range(1, chips):
            sent(gathered.at[:, q], ax_send.at[d - 1])
            sent(incoming.at[:, d], rx_send.at[d - 1])
        sent(outgoing, ad_send.at[0])
        sent(outgoing, rd_send.at[0])

    def later_section():
        tiles = group // 2
        for k in range(cuts[0]):
            query_load(0, k).wait()
            for d in range(1, chips):
                x_copy(0, d, k, q).start()
        transpose_out()
        rounds = [(kind, k) for kind in range(3) for k in range(cuts[kind])]
        outs = rounds[cuts[0]:]

        def send_out(one):
            for d in range(1, chips):
                x_copy(one[0], d, one[1], q).start()

        for one in outs[:AHEAD]:
            send_out(one)

        @pl.when(sec > 1)
        def _():
            for one in outs[AHEAD:]:
                send_out(one)

        for j in range(1, groups):
            for k in range(cuts[0]):
                query_load(j, k).wait()
        for kind in range(2):
            own_copy(kind, q).start()
        tables(q)
        for off in range(1, depth + 1):

            @pl.when(q < off)
            def _():
                window[:, off - 1] = jnp.zeros((micro, keep, 2 * kv_width), BF16)

        for h in range(kv_heads):
            for b in range(2):
                sink_rows[2 * h + b:2 * h + b + 1, :] = sink_row(h * group + b, tiles)
        pair_load.wait()

        def forward(kind, k):
            for d in range(1, chips):
                x_copy(kind, d, k, source(d, core)).wait_recv()
                if kind < 2:
                    for e in range(1, groups):
                        y_copy(kind, d, k, e, source(d, core), g).start()
                d_copy(kind, d, k, 0, source(d, core)).start()

        def relay(kind, k):
            if kind < 2:
                for d in range(1, chips):
                    for e in range(1, groups):
                        y_copy(kind, d, k, e, source(d, core), (g - e + groups) % groups).wait_recv()
                        d_copy(kind, d, k, e, source(d, core)).start()

        def several(first, size):
            return out_w.at[pl.ds(0, (chips - 1) * shard), pl.ds(first, size)]

        def ready_queries():
            own_copy(0, partner).wait_recv()
            if chips > 1:
                landed(query_w.at[pl.ds(0, chips - 1)], d_recv.at[0])

        def ready(k):
            if k == 0:
                own_copy(1, partner).wait_recv()
            if chips > 1:
                landed(several(*out_edges[k]), d_recv.at[1 + k])

        def gather_sent():
            for kind in range(3):
                for d in range(1, chips):
                    sent(part_of(kind, q, g), x_send.at[kind, d - 1])
                    for e in range(1, groups if kind < 2 else 1):
                        sent(part_of(kind, source(d, core), g), y_send.at[kind, d - 1, e - 1])
            if chips > 1:
                sent(query_w.at[pl.ds(0, chips - 1)], d_send.at[0])
                sent(several(0, last_edge[0]), d_send.at[1])
                sent(several(*last_edge), d_send.at[2])
            for kind in range(2):
                own_copy(kind, q).wait_send()

        def enter(t):
            landed(arrive.at[t], z_recv.at[t])
            normed_ref[t] = norm(arrive[t])
            cache_of(t, normed_ref[t], cos_tab[mine], sin_tab[mine], True)

        def ask(t):
            normed = normed_ref[t]
            cosine, sine = cos_tab[mine], sin_tab[mine]
            for s in range(seq):
                queries = jnp.dot(normed, query_w[s], preferred_element_type=F32)
                for p in range(shard // LANES):
                    rotated = rotate(queries[:, p * LANES:(p + 1) * LANES], cosine, sine) * 0.125
                    qbuf[:, s * shard + p * LANES:s * shard + (p + 1) * LANES] = rotated.astype(BF16)

        def attend(t):
            length = length_of(t)
            for off in range(1, depth + 1):

                @pl.when(q >= off)
                def _():
                    landed(window.at[t, off - 1], w_recv.at[t, off - 1])

            bias = bias_of(q, length, tiles * rows)

            def span_of(first, size):
                at = slice(first, first + size)
                parts = [window[t, off - 1, :, at] for off in range(depth, 0, -1)]
                return jnp.concatenate(parts + [cache_ref[t, :, at]], 0)

            jobs = []
            for pair in range(kv_heads // 2):
                values_t = span_of(kv_width + pair * LANES, LANES).T
                for e in range(2):
                    h = pair * 2 + e
                    head = span_of(h * HEAD_DIM, HEAD_DIM)
                    jobs.append((
                        [qbuf[:, a:a + LANES] for a in range(h * tiles * LANES, (h + 1) * tiles * LANES, LANES)],
                        jnp.concatenate([head, head], 1),
                        values_t[e * HEAD_DIM:(e + 1) * HEAD_DIM], bias,
                        [sink_rows[2 * h + b:2 * h + b + 1, :] for b in range(2)],
                    ))
            for h, some in enumerate(attention(jobs)):
                for p in range(tiles):
                    at = (h * tiles + p) * LANES
                    cbuf[t, :, at:at + LANES] = some[p * rows:(p + 1) * rows]

        def leave(t, edge, send):
            first, size = edge
            columns = slice(first, first + size)
            output = jnp.dot(cbuf[t], out_w[:, columns], preferred_element_type=F32)
            hidden_ref[t, :, columns] = (arrive[t, :, columns].astype(F32) + output).astype(BF16)
            if send:
                z_copy(t, edges.index(edge)).start()

        needed = [[] for c in range(HOP_CUTS)]
        for k, (first, size) in enumerate(out_edges):
            needed[first // step].append(k)

        @pl.when(sec == 1)
        def _():
            waiting, relayed = list(rounds), []

            def forward_next():
                if waiting:
                    one = waiting.pop(0)
                    forward(*one)
                    at = rounds.index(one) + AHEAD
                    if one[0] and at < len(rounds):
                        send_out(rounds[at])
                    relayed.append(one)

            def relay_next():
                if relayed:
                    relay(*relayed.pop(0))

            while len(waiting) > len(outs) - 2:
                forward_next()
                if len(relayed) > 1:
                    relay_next()
            while relayed and relayed[0][0] == 0:
                relay_next()
            ready_queries()
            for what in SECOND_ORDER:
                if what[0] == "f":
                    forward_next()
                elif what[0] == "r":
                    relay_next()
                elif what[0] == "w":
                    for k in needed[int(what[1])]:
                        ready(k)
                elif what[0] == "o":
                    leave(int(what[1]), edges[int(what[2])], False)

                    @pl.when(sec + 1 < sections)
                    def _():
                        z_copy(int(what[1]), int(what[2])).start()

                else:
                    (enter, ask, attend)["eqa".index(what[0])](int(what[1]))

        @pl.when(sec > 1)
        def _():
            previous = None
            for one in rounds:
                forward(*one)
                if previous is not None:
                    relay(*previous)
                previous = one
            relay(*previous)
            ready_queries()
            for k in range(len(out_edges)):
                ready(k)
            gather_sent()

        def slot(send, t, carry):
            enter(t)
            ask(t)
            attend(t)
            for edge in edges if send else [(0, width)]:
                leave(t, edge, send)
            return carry

        start = jnp.where(sec == 1, 2, 0)

        @pl.when(sec + 1 < sections)
        def _():
            lax.fori_loop(start, micro, functools.partial(slot, True), 0)

        @pl.when(sec + 1 == sections)
        def _():
            lax.fori_loop(start, micro, functools.partial(slot, False), 0)

        @pl.when(sec == 1)
        def _():
            gather_sent()

        for off in range(1, depth + 1):

            @pl.when(q + off < seq)
            def _():
                sent(window.at[:, off - 1], w_send.at[off - 1])

    @pl.when(sec == 0)
    def _():
        first_section()

    @pl.when(sec > 0)
    def _():
        later_section()

    @pl.when(sec + 1 < sections)
    def _():
        sent(arrive, z_send.at[0])


def per_device(
    shape,
    tokens, block_order, prompt_lengths, norm_gain, w_query, w_key_value, w_out, sink_logits
):
    groups, sections, seq = shape
    micro, rows, width = tokens.shape
    shard = w_query.shape[2]
    pair_width = w_key_value.shape[2]
    kv_heads = pair_width // 2 // HEAD_DIM
    lanes = seq * shard // (pair_width // 2) // 2 * rows
    chips = seq // 2
    keep = min(WIN, rows)
    depth = WIN // keep
    others, peers = max(1, chips - 1), max(1, groups - 1)
    queries = len(query_pieces(width // groups))
    rounds = queries + len(out_pieces(width))
    limit = 55488512 if seq * rows <= 512 else 57 * 1024 * 1024
    heads = sink_logits.shape[1]
    small = jnp.pad(norm_gain, ((0, 0), (0, heads + 2 * micro)))
    small = small + jnp.pad(sink_logits, ((0, 0), (width, 2 * micro)))
    places = jnp.pad(block_order[None], ((0, 0), (width + heads, micro)))
    places = places + jnp.pad(prompt_lengths[None], ((0, 0), (width + heads + micro, 0)))
    small = small + places.astype(F32)
    dma = pltpu.SemaphoreType.DMA
    vmem = pl.BlockSpec(memory_space=pltpu.VMEM)
    smem = pl.BlockSpec(memory_space=pltpu.SMEM)
    hbm = pl.BlockSpec(memory_space=pltpu.HBM)
    hidden, cache = pl.pallas_call(
        functools.partial(kernel, shape),
        out_shape=(
            jax.ShapeDtypeStruct((micro, rows, width), BF16),
            jax.ShapeDtypeStruct((micro, rows, pair_width), BF16),
        ),
        in_specs=[smem, vmem] + [hbm] * 4,
        out_specs=(vmem, vmem),
        scratch_shapes=[
            pltpu.VMEM((micro, rows, width), BF16),
            pltpu.VMEM((width, pair_width), BF16),
            pltpu.VMEM((width, shard), BF16),
            pltpu.VMEM((seq * rows, LANES), F32),
            pltpu.VMEM((seq * rows, LANES), F32),
            pltpu.VMEM((seq, width, shard), BF16),
            pltpu.VMEM((seq * shard, width), BF16),
            pltpu.VMEM((micro, rows, width), BF16),
            pltpu.VMEM((micro, depth, keep, pair_width), BF16),
            pltpu.VMEM((micro, rows, width), BF16),
            pltpu.VMEM((micro, rows, width), BF16),
            pltpu.VMEM((rows, seq * shard), BF16),
            pltpu.VMEM((micro, rows, seq * shard), BF16),
            pltpu.VMEM((2 * kv_heads, lanes), F32),
            pltpu.VMEM((micro, seq, rows, width), BF16),
            pltpu.VMEM((seq * rows, shard), BF16),
            pltpu.VMEM((WIN + seq * rows, LANES), BF16),
            pltpu.VMEM((WIN + seq * rows, LANES), BF16),
            pltpu.VMEM((seq, rows, shard), BF16),
            pltpu.VMEM((micro, chips, rows, width), BF16),
            pltpu.VMEM((micro, chips, rows, width), BF16),
            pltpu.VMEM((micro, chips, rows, width), BF16),
            pltpu.VMEM((micro, rows, width), F32),
            dma((groups * queries + 3,)),
            dma((3, others)),
            dma((others, rounds)),
            dma((3, others, peers)),
            dma((others, rounds, peers)),
            dma((3,)),
            dma((1 + rounds - queries,)),
            dma((2,)),
            dma((2,)),
            dma((depth,)),
            dma((micro, depth)),
            dma((1,)),
            dma((micro,)),
            dma((others,)),
            dma((micro, others)),
            dma((1,)),
            dma((micro,)),
            dma((1,)),
            dma((micro, chips)),
            dma((others,)),
            dma((micro, others, HOP_CUTS)),
        ],
        compiler_params=pltpu.CompilerParams(
            collective_id=0, has_side_effects=True, vmem_limit_bytes=limit
        ),
    )(
        small, small,
        tokens, w_key_value[0], w_query[0], w_out[0].T,
    )
    return hidden[None], cache[None]


def solution(mesh):
    in_specs = (
        P("groups", "seq", None),
        P("groups"),
        P("groups"),
        P("section", None),
        P("section", None, "seq"),
        P("section", None, None),
        P("section", "seq", None),
        P("section", None),
    )
    out_specs = (P("section", "groups", "seq", None), P("section", "groups", "seq", None))
    shape = tuple(mesh.shape[name] for name in ("groups", "section", "seq"))
    return jax.shard_map(
        functools.partial(per_device, shape),
        mesh=mesh, in_specs=in_specs, out_specs=out_specs, check_vma=False,
    )
```

```python
import functools
import math

import jax
import jax.numpy as jnp
from jax import lax
from jax.experimental import pallas as pl
from jax.experimental.pallas import tpu as pltpu
from jax.sharding import PartitionSpec as P

HEAD_DIM = 64
WIN = 128
LANES = 128
THETA = 150000.0
EPSILON = 1e-05
MESH = pl.DeviceIdType.MESH
F32 = jnp.float32
BF16 = jnp.bfloat16
QUERY_CUTS = 5
OUT_STEP = 256
HOP_CUTS = 3
SECOND_ORDER = (
    "e0", "f", "q0", "r", "f", "r", "f", "f", "a0", "w0", "o00", "r",
    "e1", "r", "q1", "w1", "o01", "r", "f", "w2", "o02", "a1", "o10", "o11", "o12",
)
AHEAD = 4


def query_pieces(length):
    size = length // QUERY_CUTS
    small = size // 3
    edges = [(0, small), (small, size - small)]
    return edges + [(k * size, size) for k in range(1, QUERY_CUTS)]


def out_pieces(width):
    direct = width % LANES + LANES
    coarse = (width - direct) // OUT_STEP * OUT_STEP
    edges = [(c, OUT_STEP) for c in range(0, coarse - OUT_STEP, OUT_STEP)]
    edges += [(c, LANES) for c in range(coarse - OUT_STEP, width - direct, LANES)]
    return edges + [(width - direct, direct)]


def kernel(
    shape,
    small_ref, small_row,
    tokens_hbm, pair_hbm, query_hbm, out_hbm,
    hidden_ref, cache_ref,
    tokens_ref, pair_ref, out_t, cos_tab, sin_tab,
    query_w, out_w, arrive, window, hbuf, normed_ref, qbuf, cbuf, sink_rows,
    gathered, tq, kd_buf, vd_buf, ctx, outgoing, incoming, final, acc,
    local_sem, x_send, x_recv, y_send, y_recv, d_send, d_recv, own_send, own_recv,
    w_send, w_recv, z_send, z_recv,
    ax_send, ax_recv, ad_send, ad_recv, rd_send, rd_recv, rx_send, rx_recv,
):
    groups, sections, seq = shape
    chips = seq // 2
    g = lax.axis_index("groups")
    sec = lax.axis_index("section")
    q = lax.axis_index("seq")
    chip, core = q // 2, q % 2
    partner = chip * 2 + (1 - core)
    micro, rows, width = hidden_ref.shape
    shard = query_w.shape[2]
    heads_width = seq * shard
    kv_width = pair_ref.shape[1] // 2
    kv_heads = kv_width // HEAD_DIM
    group = heads_width // kv_width
    keep = min(WIN, rows)
    depth = WIN // keep
    span = WIN + rows
    total = seq * rows
    half = HEAD_DIM // 2
    own_heads = shard // HEAD_DIM

    query_rows = width // groups
    query_edges = query_pieces(query_rows)
    out_rows = shard // groups
    out_edges = out_pieces(width)
    last_edge = out_edges[-1]
    cuts = (len(query_edges), len(out_edges) - 1, 1)

    def query_load(j, k):
        first = pl.multiple_of(((g + j) % groups) * query_rows + query_edges[k][0], 16)
        size = query_edges[k][1]
        return pltpu.make_async_copy(
            query_hbm.at[pl.ds(first, size)], query_w.at[q, pl.ds(first, size)],
            local_sem.at[j * cuts[0] + k],
        )

    base = groups * cuts[0]
    out_load = pltpu.make_async_copy(out_hbm, out_t, local_sem.at[base])
    pair_load = pltpu.make_async_copy(pair_hbm, pair_ref, local_sem.at[base + 1])
    tokens_load = pltpu.make_async_copy(tokens_hbm, tokens_ref, local_sem.at[base + 2])

    @pl.when(sec == 0)
    def _():
        tokens_load.start()

    for j in range(groups):
        for k in range(cuts[0]):
            query_load(j, k).start()
    out_load.start()
    pair_load.start()

    barrier = pltpu.get_barrier_semaphore()
    greeted = 0
    for d in range(1, seq):
        pl.semaphore_signal(barrier, 1, device_id={"seq": (q + d) % seq}, device_id_type=MESH)
        greeted += 1
    for e in range(1, groups):
        pl.semaphore_signal(barrier, 1, device_id={"groups": (g + e) % groups}, device_id_type=MESH)
        greeted += 1
    for s in sorted({1 % sections, (sections - 1) % sections} - {0}):
        pl.semaphore_signal(barrier, 1, device_id={"section": (sec + s) % sections}, device_id_type=MESH)
        greeted += 1
    pl.semaphore_wait(barrier, greeted)

    def remote(src, dst, send, recv, target):
        return pltpu.make_async_remote_copy(
            src_ref=src, dst_ref=dst, send_sem=send, recv_sem=recv,
            device_id=target, device_id_type=MESH,
        )

    def source(d, which):
        return ((chip - d + chips) % chips) * 2 + which

    def ahead(d, which):
        return ((chip + d) % chips) * 2 + which

    def own_rows(owner):
        return pl.ds(pl.multiple_of(owner * shard, shard), shard)

    def piece(kind, owner, part, k):
        if kind == 0:
            first = part * query_rows + query_edges[k][0]
            return query_w.at[owner, pl.ds(pl.multiple_of(first, 16), query_edges[k][1])]
        if kind == 2:
            return out_w.at[own_rows(owner), pl.ds(*last_edge)]
        first = pl.multiple_of(owner * shard + part * out_rows, out_rows)
        return out_w.at[pl.ds(first, out_rows), pl.ds(*out_edges[k])]

    def whole(kind, owner):
        if kind == 0:
            return query_w.at[owner]
        return out_w.at[own_rows(owner)]

    slots = (0, cuts[0], cuts[0] + cuts[1])

    def x_copy(kind, d, k, owner):
        ref = piece(kind, owner, g, k)
        return remote(ref, ref, x_send.at[kind, d - 1], x_recv.at[d - 1, slots[kind] + k], {"seq": ahead(d, core)})

    def y_copy(kind, d, k, e, owner, part):
        ref = piece(kind, owner, part, k)
        return remote(
            ref, ref, y_send.at[kind, d - 1, e - 1], y_recv.at[d - 1, slots[kind] + k, e - 1], {"groups": (g + e) % groups}
        )

    def d_copy(kind, d, k, e, owner):
        ref = piece(kind, owner, (g - e + groups) % groups, k)
        return remote(ref, ref, d_send.at[kind], d_recv.at[0 if kind == 0 else slots[kind] - slots[1] + 1 + k], {"seq": partner})

    def part_of(kind, owner, part):
        if kind == 0:
            return query_w.at[owner, pl.ds(pl.multiple_of(part * query_rows, 16), query_rows)]
        if kind == 2:
            return piece(2, owner, part, 0)
        first = pl.multiple_of(owner * shard + part * out_rows, out_rows)
        return out_w.at[pl.ds(first, out_rows), pl.ds(0, last_edge[0])]

    def sent(ref, sem):
        remote(ref, ref, sem, sem, {"seq": partner}).wait_send()

    def landed(ref, sem):
        remote(ref, ref, sem, sem, {"seq": partner}).wait_recv()

    def own_copy(kind, owner):
        ref = whole(kind, owner)
        return remote(ref, ref, own_send.at[kind], own_recv.at[kind], {"seq": partner})

    step = -(-width // (HOP_CUTS * LANES)) * LANES
    edges = [(c * step, min(step, width - c * step)) for c in range(HOP_CUTS)]

    def z_copy(t, c):
        columns = pl.ds(*edges[c])
        return remote(
            hidden_ref.at[t, :, columns], arrive.at[t, :, columns],
            z_send.at[0], z_recv.at[t], {"section": (sec + 1) % sections},
        )

    def w_copy(t, off):
        return remote(
            cache_ref.at[t, pl.ds(rows - keep, keep)], window.at[t, off - 1],
            w_send.at[off - 1], w_recv.at[t, off - 1], {"seq": (q + off) % seq},
        )

    def ax_copy(t, d, owner):
        ref = gathered.at[t, owner]
        return remote(ref, ref, ax_send.at[d - 1], ax_recv.at[t, d - 1], {"seq": ahead(d, core)})

    def ad_copy(t, d, owner):
        ref = gathered.at[t, owner]
        return remote(ref, ref, ad_send.at[0], ad_recv.at[t], {"seq": partner})

    def rd_copy(t, d):
        return remote(
            outgoing.at[t, d], incoming.at[t, d], rd_send.at[0], rd_recv.at[t, d], {"seq": partner}
        )

    def rx_copy(t, d, c):
        columns = pl.ds(*edges[c])
        return remote(
            incoming.at[t, d, :, columns], final.at[t, d, :, columns],
            rx_send.at[d - 1], rx_recv.at[t, d - 1, c], {"seq": ahead(d, core)},
        )

    after = width + heads_width // HEAD_DIM

    def order_of(t):
        return small_ref[0, after + t]

    def length_of(t):
        length = small_ref[0, after + micro]
        for b in range(1, micro):
            length = jnp.where(order_of(t) == b, small_ref[0, after + micro + b], length)
        return length

    def tables(r):
        lane = lax.broadcasted_iota(jnp.int32, (rows, LANES), 1)
        place = lax.broadcasted_iota(jnp.int32, (rows, LANES), 0) + r * rows
        freq = jnp.exp((lane % half).astype(F32) * (-2.0 * math.log(THETA) / HEAD_DIM))
        angles = place.astype(F32) * freq
        at = pl.ds(pl.multiple_of(r * rows, rows), rows)
        cos_tab[at] = jnp.cos(angles)
        sine = jnp.sin(angles)
        sin_tab[at] = jnp.where((lane % HEAD_DIM) < half, -sine, sine)

    def rotate(tile, cosine, sine):
        lane = lax.broadcasted_iota(jnp.int32, tile.shape, 1)
        first_half = (lane % HEAD_DIM) < half
        swapped = jnp.where(
            first_half, pltpu.roll(tile, LANES - half, 1), pltpu.roll(tile, half, 1)
        )
        return tile * cosine + swapped * sine

    def norm(h):
        widened = h.astype(F32)
        scale = lax.rsqrt(jnp.mean(widened * widened, -1, keepdims=True) + EPSILON)
        return (widened * scale * small_row[:, :width]).astype(BF16)

    def transpose_out():
        out_load.wait()
        for first in range(0, width, LANES):
            size = min(LANES, width - first)
            out_w[own_rows(q), first:first + size] = out_t[first:first + size, :].T

    def bias_of(r, length, lanes):
        key = lax.broadcasted_iota(jnp.int32, (span, lanes), 0) - WIN
        row = lax.broadcasted_iota(jnp.int32, (span, lanes), 1) % rows
        column = key + r * rows
        allowed = (key <= row) & (row - key < WIN) & (column >= 0)
        allowed = allowed & ((column.astype(F32) < length) | (key == row))
        return jnp.where(allowed, F32(0.0), F32(-1e30))

    def sink_row(first, tiles):
        return jnp.concatenate(
            [jnp.full((1, rows), small_ref[0, width + first + 2 * p], F32) for p in range(tiles)], 1
        )

    low = lax.broadcasted_iota(jnp.int32, (span, LANES), 1) < HEAD_DIM
    ones = jnp.ones((16, span), BF16)

    def attention(jobs):
        scores = []
        for pairs, twice, _, _, _ in jobs:
            zero = jnp.zeros_like(twice)
            sides = jnp.concatenate([jnp.where(low, twice, zero), jnp.where(low, zero, twice)], 0)
            scores.append(lax.dot_general(
                sides, jnp.concatenate(pairs, 0), (((1,), (1,)), ((), ())),
                preferred_element_type=F32,
            ))
        results = []
        for (_, _, values_t, bias, sinks), score in zip(jobs, scores):
            extended = jnp.concatenate([values_t, ones], 0)
            parts = []
            for b in range(2):
                masked = score[b * span:(b + 1) * span] + bias
                top = jnp.maximum(jnp.max(masked, 0, keepdims=True), sinks[b])
                expo = jnp.exp(masked - top).astype(BF16)
                summed = jnp.dot(extended, expo, preferred_element_type=F32)
                whole_sum = summed[HEAD_DIM:HEAD_DIM + 1] + jnp.exp(sinks[b] - top)
                parts.append(summed[:HEAD_DIM] * (1.0 / whole_sum))
            results.append(jnp.concatenate(parts, 0).T.astype(BF16))
        return results

    def cache_of(t, normed, cosine, sine, send):
        keys = jnp.dot(normed, pair_ref[:, :kv_width], preferred_element_type=F32)
        for p in range(kv_width // LANES):
            tile = slice(p * LANES, (p + 1) * LANES)
            cache_ref[t, :, tile] = rotate(keys[:, tile], cosine, sine).astype(BF16)
        values = jnp.dot(normed, pair_ref[:, kv_width:], preferred_element_type=F32)
        cache_ref[t, :, kv_width:] = values.astype(BF16)
        if send:
            for off in range(1, depth + 1):

                @pl.when(q + off < seq)
                def _():
                    w_copy(t, off).start()

    mine = pl.ds(pl.multiple_of(q * rows, rows), rows)

    def first_section():
        tiles = shard // LANES
        tokens_load.wait()
        for t in range(micro):
            block = tokens_ref[0]
            for b in range(1, micro):
                block = jnp.where(order_of(t) == b, tokens_ref[b], block)
            hbuf[t] = block
            gathered[t, q] = norm(hbuf[t])
            if t < micro - 1 or micro < 3:
                for d in range(1, chips):
                    ax_copy(t, d, q).start()
            ad_copy(t, 0, q).start()
        for r in range(seq):
            tables(r)
        kd_buf[:WIN] = jnp.zeros((WIN, LANES), BF16)
        vd_buf[:WIN] = jnp.zeros((WIN, LANES), BF16)
        transpose_out()
        pair_load.wait()
        for j in range(groups):
            for k in range(cuts[0]):
                query_load(j, k).wait()
        for t in range(micro):
            cache_of(t, gathered[t, q], cos_tab[mine], sin_tab[mine], False)

        kv_head = (q * own_heads) // group
        pair_at = pl.ds(pl.multiple_of((kv_head // 2) * LANES, LANES), LANES)
        value_at = pl.ds(pl.multiple_of(kv_width + (kv_head // 2) * LANES, LANES), LANES)
        sinks = [sink_row(q * own_heads + b, tiles) for b in range(2)]

        def double(tile):
            lane = lax.broadcasted_iota(jnp.int32, tile.shape, 1)
            kept = jnp.where(lane // HEAD_DIM == kv_head % 2, tile, 0.0)
            return (kept + pltpu.roll(kept, HEAD_DIM, 1)).astype(BF16)

        def finish(t):
            rd_copy(t, 0).wait_recv()
            for c, (first, size) in enumerate(edges):
                columns = slice(first, first + size)
                joined = acc[t, :, columns] + incoming[t, 0, :, columns].astype(F32)
                for d in range(1, chips):
                    rx_copy(t, d, c).wait_recv()
                    joined = joined + final[t, d, :, columns].astype(F32)
                hidden_ref[t, :, columns] = joined.astype(BF16)
                if sections > 1:
                    z_copy(t, c).start()

        def compute(t):
            for d in range(1, chips):
                ax_copy(t, d, source(d, core)).wait_recv()
                ad_copy(t, d, source(d, core)).start()
            landed(outgoing.at[t], ad_recv.at[t])
            length = length_of(t)
            normed = gathered[t].reshape(total, width)
            cosine, sine = cos_tab[...], sin_tab[...]
            keys = jnp.dot(normed, pair_ref[:, pair_at], preferred_element_type=F32)
            kd_buf[WIN:] = double(rotate(keys, cosine, sine))
            vd_buf[WIN:] = double(jnp.dot(normed, pair_ref[:, value_at], preferred_element_type=F32))
            queries = jnp.dot(normed, query_w[q], preferred_element_type=F32)
            for p in range(tiles):
                tile = slice(p * LANES, (p + 1) * LANES)
                tq[:, tile] = (rotate(queries[:, tile], cosine, sine) * 0.125).astype(BF16)
            jobs = []
            for r in range(seq):
                at = slice(r * rows, r * rows + span)
                jobs.append((
                    [tq[r * rows:(r + 1) * rows, p * LANES:(p + 1) * LANES] for p in range(tiles)],
                    kd_buf[at], vd_buf[at].T[:HEAD_DIM], bias_of(r, length, tiles * rows), sinks,
                ))
            for r, some in enumerate(attention(jobs)):
                for p in range(tiles):
                    ctx[r, :, p * LANES:(p + 1) * LANES] = some[p * rows:(p + 1) * rows]

            if micro >= 3:

                @pl.when(t == micro - 1)
                def _():
                    finish(1)

            weights = out_w[own_rows(q), :]
            there = jnp.dot(
                jnp.concatenate([ctx[ahead(d, 1 - core)] for d in range(chips)], 0), weights,
                preferred_element_type=F32,
            )
            for d in list(range(1, chips)) + [0]:
                outgoing[t, d] = there[d * rows:(d + 1) * rows].astype(BF16)
                rd_copy(t, d).start()
            here = jnp.dot(
                jnp.concatenate([ctx[ahead(d, core)] for d in range(chips)], 0), weights,
                preferred_element_type=F32,
            )
            acc[t] = hbuf[t].astype(F32) + here[:rows]
            for d in range(1, chips):
                rd_copy(t, d).wait_recv()
                joined = here[d * rows:(d + 1) * rows] + incoming[t, d].astype(F32)
                incoming[t, d] = joined.astype(BF16)
                for c in range(HOP_CUTS):
                    rx_copy(t, d, c).start()

        @pl.loop(0, micro)
        def _(t):
            if micro >= 3:

                @pl.when(t == 2)
                def _():
                    finish(0)

            compute(t)
            if micro >= 3:

                @pl.when(t == 0)
                def _():
                    for d in range(1, chips):
                        ax_copy(micro - 1, d, q).start()

        @pl.loop(2 if micro >= 3 else 0, micro)
        def _(t):
            finish(t)

        for d in range(1, chips):
            sent(gathered.at[:, q], ax_send.at[d - 1])
            sent(incoming.at[:, d], rx_send.at[d - 1])
        sent(outgoing, ad_send.at[0])
        sent(outgoing, rd_send.at[0])

    def later_section():
        tiles = group // 2
        for k in range(cuts[0]):
            query_load(0, k).wait()
            for d in range(1, chips):
                x_copy(0, d, k, q).start()
        transpose_out()
        rounds = [(kind, k) for kind in range(3) for k in range(cuts[kind])]
        outs = rounds[cuts[0]:]

        def send_out(one):
            for d in range(1, chips):
                x_copy(one[0], d, one[1], q).start()

        for one in outs[:AHEAD]:
            send_out(one)

        @pl.when(sec > 1)
        def _():
            for one in outs[AHEAD:]:
                send_out(one)

        for j in range(1, groups):
            for k in range(cuts[0]):
                query_load(j, k).wait()
        for kind in range(2):
            own_copy(kind, q).start()
        tables(q)
        for off in range(1, depth + 1):

            @pl.when(q < off)
            def _():
                window[:, off - 1] = jnp.zeros((micro, keep, 2 * kv_width), BF16)

        for h in range(kv_heads):
            for b in range(2):
                sink_rows[2 * h + b:2 * h + b + 1, :] = sink_row(h * group + b, tiles)
        pair_load.wait()

        def forward(kind, k):
            for d in range(1, chips):
                x_copy(kind, d, k, source(d, core)).wait_recv()
                if kind < 2:
                    for e in range(1, groups):
                        y_copy(kind, d, k, e, source(d, core), g).start()
                d_copy(kind, d, k, 0, source(d, core)).start()

        def relay(kind, k):
            if kind < 2:
                for d in range(1, chips):
                    for e in range(1, groups):
                        y_copy(kind, d, k, e, source(d, core), (g - e + groups) % groups).wait_recv()
                        d_copy(kind, d, k, e, source(d, core)).start()

        def several(first, size):
            return out_w.at[pl.ds(0, (chips - 1) * shard), pl.ds(first, size)]

        def ready_queries():
            own_copy(0, partner).wait_recv()
            if chips > 1:
                landed(query_w.at[pl.ds(0, chips - 1)], d_recv.at[0])

        def ready(k):
            if k == 0:
                own_copy(1, partner).wait_recv()
            if chips > 1:
                landed(several(*out_edges[k]), d_recv.at[1 + k])

        def gather_sent():
            for kind in range(3):
                for d in range(1, chips):
                    sent(part_of(kind, q, g), x_send.at[kind, d - 1])
                    for e in range(1, groups if kind < 2 else 1):
                        sent(part_of(kind, source(d, core), g), y_send.at[kind, d - 1, e - 1])
            if chips > 1:
                sent(query_w.at[pl.ds(0, chips - 1)], d_send.at[0])
                sent(several(0, last_edge[0]), d_send.at[1])
                sent(several(*last_edge), d_send.at[2])
            for kind in range(2):
                own_copy(kind, q).wait_send()

        def enter(t):
            landed(arrive.at[t], z_recv.at[t])
            normed_ref[t] = norm(arrive[t])
            cache_of(t, normed_ref[t], cos_tab[mine], sin_tab[mine], True)

        def ask(t):
            normed = normed_ref[t]
            cosine, sine = cos_tab[mine], sin_tab[mine]
            for s in range(seq):
                queries = jnp.dot(normed, query_w[s], preferred_element_type=F32)
                for p in range(shard // LANES):
                    rotated = rotate(queries[:, p * LANES:(p + 1) * LANES], cosine, sine) * 0.125
                    qbuf[:, s * shard + p * LANES:s * shard + (p + 1) * LANES] = rotated.astype(BF16)

        def attend(t):
            length = length_of(t)
            for off in range(1, depth + 1):

                @pl.when(q >= off)
                def _():
                    landed(window.at[t, off - 1], w_recv.at[t, off - 1])

            bias = bias_of(q, length, tiles * rows)

            def span_of(first, size):
                at = slice(first, first + size)
                parts = [window[t, off - 1, :, at] for off in range(depth, 0, -1)]
                return jnp.concatenate(parts + [cache_ref[t, :, at]], 0)

            jobs = []
            for pair in range(kv_heads // 2):
                values_t = span_of(kv_width + pair * LANES, LANES).T
                for e in range(2):
                    h = pair * 2 + e
                    head = span_of(h * HEAD_DIM, HEAD_DIM)
                    jobs.append((
                        [qbuf[:, a:a + LANES] for a in range(h * tiles * LANES, (h + 1) * tiles * LANES, LANES)],
                        jnp.concatenate([head, head], 1),
                        values_t[e * HEAD_DIM:(e + 1) * HEAD_DIM], bias,
                        [sink_rows[2 * h + b:2 * h + b + 1, :] for b in range(2)],
                    ))
            for h, some in enumerate(attention(jobs)):
                for p in range(tiles):
                    at = (h * tiles + p) * LANES
                    cbuf[t, :, at:at + LANES] = some[p * rows:(p + 1) * rows]

        def leave(t, edge, send):
            first, size = edge
            columns = slice(first, first + size)
            output = jnp.dot(cbuf[t], out_w[:, columns], preferred_element_type=F32)
            hidden_ref[t, :, columns] = (arrive[t, :, columns].astype(F32) + output).astype(BF16)
            if send:
                z_copy(t, edges.index(edge)).start()

        needed = [[] for c in range(HOP_CUTS)]
        for k, (first, size) in enumerate(out_edges):
            needed[first // step].append(k)

        @pl.when(sec == 1)
        def _():
            waiting, relayed = list(rounds), []

            def forward_next():
                if waiting:
                    one = waiting.pop(0)
                    forward(*one)
                    at = rounds.index(one) + AHEAD
                    if one[0] and at < len(rounds):
                        send_out(rounds[at])
                    relayed.append(one)

            def relay_next():
                if relayed:
                    relay(*relayed.pop(0))

            while len(waiting) > len(outs) - 2:
                forward_next()
                if len(relayed) > 1:
                    relay_next()
            while relayed and relayed[0][0] == 0:
                relay_next()
            ready_queries()
            for what in SECOND_ORDER:
                if what[0] == "f":
                    forward_next()
                elif what[0] == "r":
                    relay_next()
                elif what[0] == "w":
                    for k in needed[int(what[1])]:
                        ready(k)
                elif what[0] == "o":
                    leave(int(what[1]), edges[int(what[2])], False)

                    @pl.when(sec + 1 < sections)
                    def _():
                        z_copy(int(what[1]), int(what[2])).start()

                else:
                    (enter, ask, attend)["eqa".index(what[0])](int(what[1]))

        @pl.when(sec > 1)
        def _():
            previous = None
            for one in rounds:
                forward(*one)
                if previous is not None:
                    relay(*previous)
                previous = one
            relay(*previous)
            ready_queries()
            for k in range(len(out_edges)):
                ready(k)
            gather_sent()

        def slot(send, t, carry):
            enter(t)
            ask(t)
            attend(t)
            for edge in edges if send else [(0, width)]:
                leave(t, edge, send)
            return carry

        start = jnp.where(sec == 1, 2, 0)

        @pl.when(sec + 1 < sections)
        def _():
            lax.fori_loop(start, micro, functools.partial(slot, True), 0)

        @pl.when(sec + 1 == sections)
        def _():
            lax.fori_loop(start, micro, functools.partial(slot, False), 0)

        @pl.when(sec == 1)
        def _():
            gather_sent()

        for off in range(1, depth + 1):

            @pl.when(q + off < seq)
            def _():
                sent(window.at[:, off - 1], w_send.at[off - 1])

    @pl.when(sec == 0)
    def _():
        first_section()

    @pl.when(sec > 0)
    def _():
        later_section()

    @pl.when(sec + 1 < sections)
    def _():
        sent(arrive, z_send.at[0])


def per_device(
    shape,
    tokens, block_order, prompt_lengths, norm_gain, w_query, w_key_value, w_out, sink_logits
):
    groups, sections, seq = shape
    micro, rows, width = tokens.shape
    shard = w_query.shape[2]
    pair_width = w_key_value.shape[2]
    kv_heads = pair_width // 2 // HEAD_DIM
    lanes = seq * shard // (pair_width // 2) // 2 * rows
    chips = seq // 2
    keep = min(WIN, rows)
    depth = WIN // keep
    others, peers = max(1, chips - 1), max(1, groups - 1)
    queries = len(query_pieces(width // groups))
    rounds = queries + len(out_pieces(width))
    limit = 55488512 if seq * rows <= 512 else 57 * 1024 * 1024
    heads = sink_logits.shape[1]
    small = jnp.pad(norm_gain, ((0, 0), (0, heads + 2 * micro)))
    small = small + jnp.pad(sink_logits, ((0, 0), (width, 2 * micro)))
    places = jnp.pad(block_order[None], ((0, 0), (width + heads, micro)))
    places = places + jnp.pad(prompt_lengths[None], ((0, 0), (width + heads + micro, 0)))
    small = small + places.astype(F32)
    dma = pltpu.SemaphoreType.DMA
    vmem = pl.BlockSpec(memory_space=pltpu.VMEM)
    smem = pl.BlockSpec(memory_space=pltpu.SMEM)
    hbm = pl.BlockSpec(memory_space=pltpu.HBM)
    hidden, cache = pl.pallas_call(
        functools.partial(kernel, shape),
        out_shape=(
            jax.ShapeDtypeStruct((micro, rows, width), BF16),
            jax.ShapeDtypeStruct((micro, rows, pair_width), BF16),
        ),
        in_specs=[smem, vmem] + [hbm] * 4,
        out_specs=(vmem, vmem),
        scratch_shapes=[
            pltpu.VMEM((micro, rows, width), BF16),
            pltpu.VMEM((width, pair_width), BF16),
            pltpu.VMEM((width, shard), BF16),
            pltpu.VMEM((seq * rows, LANES), F32),
            pltpu.VMEM((seq * rows, LANES), F32),
            pltpu.VMEM((seq, width, shard), BF16),
            pltpu.VMEM((seq * shard, width), BF16),
            pltpu.VMEM((micro, rows, width), BF16),
            pltpu.VMEM((micro, depth, keep, pair_width), BF16),
            pltpu.VMEM((micro, rows, width), BF16),
            pltpu.VMEM((micro, rows, width), BF16),
            pltpu.VMEM((rows, seq * shard), BF16),
            pltpu.VMEM((micro, rows, seq * shard), BF16),
            pltpu.VMEM((2 * kv_heads, lanes), F32),
            pltpu.VMEM((micro, seq, rows, width), BF16),
            pltpu.VMEM((seq * rows, shard), BF16),
            pltpu.VMEM((WIN + seq * rows, LANES), BF16),
            pltpu.VMEM((WIN + seq * rows, LANES), BF16),
            pltpu.VMEM((seq, rows, shard), BF16),
            pltpu.VMEM((micro, chips, rows, width), BF16),
            pltpu.VMEM((micro, chips, rows, width), BF16),
            pltpu.VMEM((micro, chips, rows, width), BF16),
            pltpu.VMEM((micro, rows, width), F32),
            dma((groups * queries + 3,)),
            dma((3, others)),
            dma((others, rounds)),
            dma((3, others, peers)),
            dma((others, rounds, peers)),
            dma((3,)),
            dma((1 + rounds - queries,)),
            dma((2,)),
            dma((2,)),
            dma((depth,)),
            dma((micro, depth)),
            dma((1,)),
            dma((micro,)),
            dma((others,)),
            dma((micro, others)),
            dma((1,)),
            dma((micro,)),
            dma((1,)),
            dma((micro, chips)),
            dma((others,)),
            dma((micro, others, HOP_CUTS)),
        ],
        compiler_params=pltpu.CompilerParams(
            collective_id=0, has_side_effects=True, vmem_limit_bytes=limit
        ),
    )(
        small, small,
        tokens, w_key_value[0], w_query[0], w_out[0].T,
    )
    return hidden[None], cache[None]


def solution(mesh):
    in_specs = (
        P("groups", "seq", None),
        P("groups"),
        P("groups"),
        P("section", None),
        P("section", None, "seq"),
        P("section", None, None),
        P("section", "seq", None),
        P("section", None),
    )
    out_specs = (P("section", "groups", "seq", None), P("section", "groups", "seq", None))
    shape = tuple(mesh.shape[name] for name in ("groups", "section", "seq"))
    return jax.shard_map(
        functools.partial(per_device, shape),
        mesh=mesh, in_specs=in_specs, out_specs=out_specs, check_vma=False,
    )
```
